32 devices in a mesh: dp: 4 (over x, core), fsdp: 8 (over z, y).
Axes of the slice: x: 2, y: 2, z: 4, core: 2. Of those that a mesh axis runs over, the one named last changes fastest.
Arguments:
- text_rows: bfloat16 [64, 512, 768], P(('dp', 'fsdp')), may hold values from -6 to 6
- visual_matrix: bfloat16 [768, 768], P('fsdp'), may hold values from -0.21875 to 0.21875
- batch_gain: bfloat16 [768], P('fsdp'), may hold values from 0.5 to 1.5
- batch_shift: bfloat16 [768], P('fsdp'), may hold values from -2.5 to 2.5
- attend_weight: bfloat16 [768, 2304], P('fsdp'), may hold values from -0.21875 to 0.21875
- merge_weight: bfloat16 [768, 768], P('fsdp'), may hold values from -1.75 to 1.75
- first_gain: bfloat16 [768], P('fsdp'), may hold values from 0.5 to 1.5
- first_shift: bfloat16 [768], P('fsdp'), may hold values from -2.5 to 2.5
- up_matrix: bfloat16 [768, 3072], P('fsdp'), may hold values from -0.21875 to 0.21875
- down_matrix: bfloat16 [3072, 768], P('fsdp'), may hold values from -0.109375 to 0.109375
- second_gain: bfloat16 [768], P('fsdp'), may hold values from 0.5 to 1.5
- second_shift: bfloat16 [768], P('fsdp'), may hold values from -2.5 to 2.5
- segment_counts: int32 [64], P(('dp', 'fsdp')), may hold values from 5 to 128, as said below
- segment_ids: int32 [64, 512], P(('dp', 'fsdp')), may hold values from -1 to 127, as said below
- padding_mask: int32 [64, 512], P(('dp', 'fsdp')), may hold values from 0 to 1, as said below
- cotangent: bfloat16 [64, 512, 768], P(('dp', 'fsdp')), may hold values from -6 to 6
Outputs:
- layer_output: float32 [64, 512, 768], P(('dp', 'fsdp'))
- text_gradient: float32 [64, 512, 768], P(('dp', 'fsdp'))
- visual_gradient: float32 [768, 768], P('fsdp')
- batch_gain_gradient: float32 [768], P('fsdp')
- batch_shift_gradient: float32 [768], P('fsdp')
- attend_gradient: float32 [768, 2304], P('fsdp')
- merge_gradient: float32 [768, 768], P('fsdp')
- first_gain_gradient: float32 [768], P('fsdp')
- first_shift_gradient: float32 [768], P('fsdp')
- up_gradient: float32 [768, 3072], P('fsdp')
- down_gradient: float32 [3072, 768], P('fsdp')
- second_gain_gradient: float32 [768], P('fsdp')
- second_shift_gradient: float32 [768], P('fsdp')
The draws below stay inside these ranges and needn't reach their ends.
Inputs may be any that keep to these rules, and one draw needn't show every extreme that they name: On every device of dp+fsdp one of its documents has exactly 128 segments; segment_counts[d] is one more than the largest segment_ids in document d. `segment_ids`: A document's real rows come first and form segment_counts consecutive runs of one or more rows, numbered 0, 1, ... in order; padding rows hold -1. `padding_mask`: 1 exactly on the rows whose segment id is not -1, which are the first 256 or more rows of a document.
All inputs are finite; a program needn't handle non-finite values.
Results may differ from the reference program's by a relative error of at most 0.023.
The reference program's roundings to bfloat16 on the way count: a program that leaves them out, or rounds other values in their place, can miss the bound.
Values may be sent and summed in bfloat16 or wider, within the bound.
No kernel may reach another device: no remote copies, remote signals or barrier semaphores. Data moves between devices by JAX's collectives and lax.ppermute only.
A program may use at most 192 MiB of HBM per device.

```python
import jax
import jax.numpy as jnp
from jax import lax

D = 768
HEADS = 12
HDIM = 64
FF = 3072
SEQ = 512
SEGMAX = 128
DOCS_DEV = 2
DOCS = 64


def layout(key):
    base = jax.random.fold_in(key, 101)
    subkeys = jax.random.split(base, 5)
    spread = SEGMAX - 5
    left_factor = jax.random.randint(subkeys[0], (DOCS,), 0, spread + 1)
    right_factor = jax.random.randint(subkeys[1], (DOCS,), 0, spread + 1)
    counts = 5 + left_factor * right_factor // spread
    owners = DOCS // DOCS_DEV
    chosen = jax.random.randint(subkeys[2], (owners,), 0, DOCS_DEV)
    doc_index = jnp.arange(DOCS)
    forced = doc_index % DOCS_DEV == jnp.repeat(chosen, DOCS_DEV, total_repeat_length=DOCS)
    counts = jnp.where(forced, SEGMAX, counts)
    lengths = SEQ // 2 + jax.random.randint(subkeys[3], (DOCS,), 0, SEQ // 2 + 1)
    row_index = jnp.arange(SEQ)
    eligible = (row_index[None, :] >= 1) & (row_index[None, :] < lengths[:, None])
    raw_scores = jax.random.randint(subkeys[4], (DOCS, SEQ), 0, 1 << 20) * SEQ + row_index[None, :]
    ranked_scores = jnp.where(eligible, raw_scores, -1 - row_index[None, :])
    sorted_order = jnp.argsort(-ranked_scores, axis=1)
    position_rank = jnp.argsort(sorted_order, axis=1)
    boundary = (position_rank < counts[:, None] - 1).astype(jnp.int32)
    segment_of = jnp.cumsum(boundary, axis=1)
    valid_row = row_index[None, :] < lengths[:, None]
    segment_of = jnp.where(valid_row, segment_of, -1)
    return (counts.astype(jnp.int32), segment_of.astype(jnp.int32), valid_row.astype(jnp.int32))


def draw_segment_counts(key, part):
    return layout(key)[0]


def draw_segment_ids(key, part):
    return layout(key)[1]


def draw_padding_mask(key, part):
    return layout(key)[2]


def shard_levels(stream_key, dims, cuts, low, high):
    def one(dim, parts):
        draws = jax.random.uniform(jax.random.fold_in(jax.random.fold_in(stream_key, 6), dim), (parts,), jnp.float32, low / len(cuts), high / len(cuts))
        return jnp.repeat(jnp.exp(draws), dims[dim] // parts).reshape((-1,) + (1,) * (len(dims) - dim - 1))

    level = one(*cuts[0])
    for cut in cuts[1:]:
        level = level * one(*cut)
    return level


def normal_values(rng, dims, scale, most, cuts=(), dtype=jnp.bfloat16):
    factor_of = shard_levels(rng, dims, cuts, -0.22, 0.18) if cuts else 1.0
    values = jax.random.normal(rng, dims, jnp.float32) * scale * factor_of
    return jnp.minimum(jnp.maximum(values, -most), most).astype(dtype)


def setup_inputs(seed: int = 0) -> dict:
    keys = jax.random.split(jax.random.key(seed), 17)
    text_rows = normal_values(keys[0], (DOCS, SEQ, D), 1.0, 6.0, ((0, 32),))
    visual_matrix = normal_values(keys[1], (D, D), D ** -0.5, 0.21875, ((0, 8),))
    batch_gain = jnp.clip(1.0 + 0.1 * jax.random.normal(keys[2], (D,), jnp.float32), 0.5, 1.5).astype(jnp.bfloat16)
    batch_shift = normal_values(keys[3], (D,), 0.3, 2.5, ((0, 8),))
    attend_weight = normal_values(keys[4], (D, 3 * D), D ** -0.5, 0.21875, ((0, 8),))
    merge_weight = normal_values(keys[5], (D, D), (max(D // 64, 1)) ** -0.5, 1.75, ((0, 8),))
    first_gain = jnp.clip(1.0 + 0.1 * jax.random.normal(keys[6], (D,), jnp.float32), 0.5, 1.5).astype(jnp.bfloat16)
    first_shift = normal_values(keys[7], (D,), 0.3, 2.5, ((0, 8),))
    up_matrix = normal_values(keys[8], (D, FF), D ** -0.5, 0.21875, ((0, 8),))
    down_matrix = normal_values(keys[9], (FF, D), FF ** -0.5, 0.109375, ((0, 8),))
    second_gain = jnp.clip(1.0 + 0.1 * jax.random.normal(keys[10], (D,), jnp.float32), 0.5, 1.5).astype(jnp.bfloat16)
    second_shift = normal_values(keys[11], (D,), 0.3, 2.5, ((0, 8),))
    segment_counts = draw_segment_counts(jax.random.fold_in(keys[16], 71), 0)
    segment_ids = draw_segment_ids(jax.random.fold_in(keys[16], 71), 0)
    padding_mask = draw_padding_mask(jax.random.fold_in(keys[16], 71), 0)
    cotangent = normal_values(keys[15], (DOCS, SEQ, D), 1.0, 6.0, ((0, 32),))
    return {"text_rows": text_rows, "visual_matrix": visual_matrix, "batch_gain": batch_gain, "batch_shift": batch_shift, "attend_weight": attend_weight, "merge_weight": merge_weight, "first_gain": first_gain, "first_shift": first_shift, "up_matrix": up_matrix, "down_matrix": down_matrix, "second_gain": second_gain, "second_shift": second_shift, "segment_counts": segment_counts, "segment_ids": segment_ids, "padding_mask": padding_mask, "cotangent": cotangent}


@jax.custom_vjp
def reduced_precision(v):
    return lax.optimization_barrier(v.astype(jnp.bfloat16)).astype(jnp.float32)

@jax.custom_vjp
def reduced_backward(v):
    return v

def low_keep(v):
    return (reduced_precision(v), None)

def low_pass(kept, grad):
    return (grad,)

def back_keep(v):
    return (v, None)

def back_low(kept, grad):
    return (reduced_precision(grad),)
reduced_precision.defvjp(low_keep, low_pass)
reduced_backward.defvjp(back_keep, back_low)
eps_norm = 1e-05
eps_batch = 1e-05
masked_score = -1e+30
group_docs = 8
highest_precision = lax.Precision.HIGHEST

def layer_norm(values, gain, shift):
    center = values - lax.optimization_barrier(jnp.mean(values, axis=-1, keepdims=True))
    variance = lax.optimization_barrier(jnp.mean(center * center, axis=-1, keepdims=True))
    return center * lax.rsqrt(variance + eps_norm) * gain + shift

def pool_group(operands, visual_matrix):
    text_group, segment_group = operands
    slot_index = jnp.arange(SEGMAX)
    onehot = (segment_group[:, :, None] == slot_index[None, None, :]).astype(jnp.float32)
    rowcount = lax.optimization_barrier(jnp.sum(onehot, axis=1))
    sums = jnp.einsum('drs,drc->dsc', onehot, text_group, precision=highest_precision)
    pooled_segments = sums / jnp.maximum(rowcount, 1.0)[..., None]
    return reduced_backward(jnp.einsum('bil,ly->biy', reduced_precision(pooled_segments), visual_matrix, precision=highest_precision))

def encode_group(operands, weights):
    text_group, embed_group, segment_group, mask_group = operands
    attend_weight, merge_weight, first_gain, first_shift, up_matrix, down_matrix, second_gain, second_shift = weights
    slot_index = jnp.arange(SEGMAX)
    onehot = (segment_group[:, :, None] == slot_index[None, None, :]).astype(jnp.float32)
    joined = text_group + jnp.einsum('drs,dsc->drc', onehot, embed_group, precision=highest_precision)
    packed = reduced_backward(reduced_precision(jnp.einsum('drc,ce->dre', reduced_precision(joined), attend_weight, precision=highest_precision)))
    length = joined.shape[1]
    queries = packed[..., :D].reshape(group_docs, length, HEADS, HDIM)
    keys_part = packed[..., D:2 * D].reshape(group_docs, length, HEADS, HDIM)
    values_part = packed[..., 2 * D:].reshape(group_docs, length, HEADS, HDIM)
    scores = reduced_backward(jnp.einsum('dqhe,dkhe->dhqk', queries, keys_part, precision=highest_precision) * HDIM ** (-0.5))
    scores = jnp.where(mask_group[:, None, None, :] > 0, scores, masked_score)
    attention = jax.nn.softmax(scores, axis=-1)
    mixed = jnp.einsum('dhqk,dkhe->dqhe', reduced_precision(attention), values_part, precision=highest_precision)
    attended = reduced_backward(reduced_precision(mixed.reshape(group_docs, length, D)))
    projected = reduced_backward(jnp.einsum('drc,ce->dre', attended, merge_weight, precision=highest_precision))
    hidden_state = layer_norm(joined + projected, first_gain, first_shift)
    inner_hidden = reduced_backward(jnp.einsum('sjq,qy->sjy', reduced_precision(hidden_state), up_matrix, precision=highest_precision))
    gelu_activated = reduced_precision(jax.nn.gelu(inner_hidden, approximate=False))
    residual_branch = reduced_backward(jnp.einsum('zya,av->zyv', gelu_activated, down_matrix, precision=highest_precision))
    return layer_norm(hidden_state + residual_branch, second_gain, second_shift)

def forward(text_rows, visual_matrix, batch_gain, batch_shift, attend_weight, merge_weight, first_gain, first_shift, up_matrix, down_matrix, second_gain, second_shift, segment_counts, segment_ids, padding_mask):
    groups = DOCS // group_docs
    text_groups = text_rows.reshape(groups, group_docs, SEQ, D)
    segment_groups = segment_ids.reshape(groups, group_docs, SEQ)
    mask_groups = padding_mask.reshape(groups, group_docs, SEQ)

    def pool_one(operands):
        return pool_group(operands, visual_matrix)
    visual_rows = lax.map(jax.checkpoint(pool_one), (text_groups, segment_groups)).reshape(DOCS, SEGMAX, D)
    valid_slot = (jnp.arange(SEGMAX)[None, :] < segment_counts[:, None]).astype(jnp.float32)[..., None]
    segment_total = jnp.sum(segment_counts).astype(jnp.float32)
    batch_center = lax.optimization_barrier(jnp.sum(valid_slot * visual_rows, axis=(0, 1))) / segment_total
    center = visual_rows - batch_center
    variance = lax.optimization_barrier(jnp.sum(valid_slot * center * center, axis=(0, 1))) / segment_total
    normed = center * lax.rsqrt(variance + eps_batch)
    embedded = reduced_precision(normed * batch_gain + batch_shift)
    weights = (attend_weight, merge_weight, first_gain, first_shift, up_matrix, down_matrix, second_gain, second_shift)

    def encode_one(operands):
        return encode_group(operands, weights)
    encoded = lax.map(jax.checkpoint(encode_one), (text_groups, embedded.reshape(groups, group_docs, SEGMAX, D), segment_groups, mask_groups))
    return encoded.reshape(DOCS, SEQ, D)

def reference(text_rows, visual_matrix, batch_gain, batch_shift, attend_weight, merge_weight, first_gain, first_shift, up_matrix, down_matrix, second_gain, second_shift, segment_counts, segment_ids, padding_mask, cotangent):
    floats = tuple((array.astype(jnp.float32) for array in (text_rows, visual_matrix, batch_gain, batch_shift, attend_weight, merge_weight, first_gain, first_shift, up_matrix, down_matrix, second_gain, second_shift)))

    def wrapped(*operands):
        return forward(*operands, segment_counts, segment_ids, padding_mask)
    layer_output, pullback = jax.vjp(wrapped, *floats)
    gradients = pullback(cotangent.astype(jnp.float32))
    return (layer_output, gradients[0], gradients[1], gradients[2], gradients[3], gradients[4], gradients[5], gradients[6], gradients[7], gradients[8], gradients[9], gradients[10], gradients[11])
```

```python
import jax
import jax.numpy as jnp
from jax import lax
from jax.sharding import PartitionSpec as P

HEADS = 12
SEGMAX = 128
low = jnp.bfloat16


def pair_groups(size):
    return [[i, i + 1] for i in range(0, size, 2)]


def line_groups(size):
    return [list(range(0, size, 2)), list(range(1, size, 2))]


def spread(value, axis, groups, count):
    copies = jnp.broadcast_to(value[None], (count,) + value.shape)
    return lax.all_to_all(copies, axis, 0, 0, axis_index_groups=groups)


def gather_weight(shard):
    rows, columns = shard.shape
    dp, fsdp = lax.axis_size("dp"), lax.axis_size("fsdp")
    half = columns // 2
    core = lax.axis_index("dp") % 2
    mine = lax.dynamic_slice_in_dim(shard, core * half, half, 1)
    line = spread(mine, "fsdp", line_groups(fsdp), fsdp // 2)
    both = spread(line, "fsdp", pair_groups(fsdp), 2)
    full = spread(both, "dp", pair_groups(dp), 2)
    full = full.transpose(2, 1, 3, 0, 4)
    return full.reshape(fsdp * rows, columns)


def gather_first(shard):
    rows, columns = shard.shape
    dp, fsdp = lax.axis_size("dp"), lax.axis_size("fsdp")
    half = columns // 2
    core = lax.axis_index("dp") % 2
    mine = lax.dynamic_slice_in_dim(shard, core * half, half, 1)
    line = spread(mine, "fsdp", None, fsdp)
    full = spread(line, "dp", pair_groups(dp), 2)
    return full.transpose(1, 2, 0, 3).reshape(fsdp * rows, columns)


def swap(value, axis, bit):
    size = lax.axis_size(axis)
    return lax.ppermute(value, axis, [(i, i ^ bit) for i in range(size)])


def add_low(left, right):
    return (left.astype(jnp.float32) + right.astype(jnp.float32)).astype(low)


def scatter_gradient(local):
    rows, columns = local.shape
    dp, fsdp = lax.axis_size("dp"), lax.axis_size("fsdp")
    half = columns // 2
    piece = rows // fsdp
    core = lax.axis_index("dp") % 2
    side = lax.axis_index("fsdp") % 2
    local = local.astype(low)
    keep = lax.dynamic_slice_in_dim(local, core * half, half, 1)
    give = lax.dynamic_slice_in_dim(local, (1 - core) * half, half, 1)
    chip = add_low(keep, swap(give, "dp", 1)).reshape(fsdp // 2, 2, piece, half)
    keep = lax.dynamic_index_in_dim(chip, side, 1, False)
    give = lax.dynamic_index_in_dim(chip, 1 - side, 1, False)
    pair = add_low(keep, swap(give, "fsdp", 1))
    parts = lax.all_to_all(pair, "fsdp", 0, 0, axis_index_groups=line_groups(fsdp))
    total = jnp.sum(parts.astype(jnp.float32), axis=0).astype(low)
    bit = 2
    while bit < dp:
        total = add_low(total, swap(total, "dp", bit))
        bit *= 2
    both = spread(total, "dp", pair_groups(dp), 2)
    return both.transpose(1, 0, 2).reshape(piece, columns).astype(jnp.float32)


def sum_all(value):
    dp, fsdp = lax.axis_size("dp"), lax.axis_size("fsdp")
    value = jnp.sum(spread(value, "fsdp", None, fsdp), axis=0)
    return jnp.sum(spread(value, "dp", None, dp), axis=0)

eps_norm = 1e-05
eps_batch = 1e-05
masked_score = -1e30
highest_precision = lax.Precision.HIGHEST


def layer_norm(values, gain, shift):
    center = values - jnp.mean(values, axis=-1, keepdims=True)
    variance = jnp.mean(center * center, axis=-1, keepdims=True)
    return center * lax.rsqrt(variance + eps_norm) * gain + shift


def exact_gelu(values):
    return jax.nn.gelu(values, approximate=False)


def split_heads(packed):
    length = packed.shape[0]
    features = packed.shape[1] // 3
    head_size = features // HEADS
    queries = packed[:, :features].reshape(length, HEADS, head_size)
    keys_part = packed[:, features : 2 * features].reshape(length, HEADS, head_size)
    values_part = packed[:, 2 * features :].reshape(length, HEADS, head_size)
    return (queries, keys_part, values_part, head_size ** (-0.5))


def masked_scores(queries, keys_part, key_mask, scaling):
    scores = (
        jnp.einsum("qhe,khe->hqk", queries, keys_part, preferred_element_type=jnp.float32) * scaling
    )
    return jnp.where(key_mask[None, None, :] > 0, scores, masked_score)


def attend_doc(operands):
    packed, key_mask = operands
    queries, keys_part, values_part, scaling = split_heads(packed)
    scores = masked_scores(queries, keys_part, key_mask, scaling)
    top_score = jnp.max(scores, axis=-1, keepdims=True)
    unnormed = jnp.exp(scores - top_score)
    totals = jnp.sum(unnormed, axis=-1, keepdims=True)
    attention = unnormed / totals
    mixed = jnp.einsum(
        "hqk,khe->qhe",
        attention.astype(jnp.bfloat16),
        values_part,
        preferred_element_type=jnp.float32,
    )
    log_total = (top_score + jnp.log(totals))[..., 0]
    return (mixed.reshape(packed.shape[0], packed.shape[1] // 3).astype(jnp.bfloat16), log_total)


def attend_back(operands):
    packed, key_mask, log_total, delta_attended = operands
    queries, keys_part, values_part, scaling = split_heads(packed)
    length = packed.shape[0]
    features = packed.shape[1] // 3
    scores = masked_scores(queries, keys_part, key_mask, scaling)
    attention = jnp.exp(scores - log_total[..., None])
    delta_heads = delta_attended.reshape(length, HEADS, features // HEADS)
    delta_attention = jnp.einsum(
        "qhe,khe->hqk", delta_heads, values_part, preferred_element_type=jnp.float32
    )
    delta_scores = attention * (
        delta_attention - jnp.sum(attention * delta_attention, axis=-1, keepdims=True)
    )
    delta_low = delta_scores.astype(jnp.bfloat16)
    delta_queries = (
        jnp.einsum("hqk,khe->qhe", delta_low, keys_part, preferred_element_type=jnp.float32)
        * scaling
    )
    delta_keys = (
        jnp.einsum("hqk,qhe->khe", delta_low, queries, preferred_element_type=jnp.float32) * scaling
    )
    delta_values = jnp.einsum(
        "hqk,qhe->khe",
        attention.astype(jnp.bfloat16),
        delta_heads,
        preferred_element_type=jnp.float32,
    )
    merged = jnp.concatenate(
        [
            delta_queries.reshape(length, features),
            delta_keys.reshape(length, features),
            delta_values.reshape(length, features),
        ],
        axis=1,
    )
    return merged.astype(jnp.bfloat16)


def shards(
    text_rows,
    visual_matrix,
    batch_gain,
    batch_shift,
    attend_weight,
    merge_weight,
    first_gain,
    first_shift,
    up_matrix,
    down_matrix,
    second_gain,
    second_shift,
    segment_counts,
    segment_ids,
    padding_mask,
    cotangent,
):
    small = jnp.stack([batch_gain, batch_shift, first_gain, first_shift, second_gain, second_shift])
    small = spread(small, "fsdp", None, lax.axis_size("fsdp"))
    small = small.transpose(1, 0, 2).reshape(6, -1)
    full_batch_gain, full_batch_shift, full_first_gain, full_first_shift, full_second_gain, full_second_shift = (
        small[i] for i in range(6)
    )
    gathered_visual_weight = gather_first(visual_matrix)
    full_attend = gather_weight(attend_weight)
    full_merge = gather_weight(merge_weight)
    gathered_up_weight = gather_weight(up_matrix)
    gathered_down_weight = gather_weight(down_matrix)
    features = text_rows.shape[2]
    slot_index = jnp.arange(SEGMAX)
    matches = segment_ids[:, :, None] == slot_index[None, None, :]
    onehot = matches.astype(jnp.bfloat16)
    onehot_wide = matches.astype(jnp.float32)
    divisor = jnp.maximum(jnp.sum(onehot_wide, axis=1), 1.0)[..., None]
    pooled_segments = (
        jnp.einsum("drs,drc->dsc", onehot, text_rows, preferred_element_type=jnp.float32) / divisor
    ).astype(jnp.bfloat16)
    visual_rows = jnp.einsum(
        "bil,ly->biy", pooled_segments, gathered_visual_weight, preferred_element_type=jnp.float32
    )
    valid_slot = (slot_index[None, :] < segment_counts[:, None]).astype(jnp.float32)[..., None]
    local_count = jnp.sum(segment_counts).astype(jnp.float32)
    local_sum = jnp.sum(valid_slot * visual_rows, axis=(0, 1))
    local_center = visual_rows - local_sum / local_count
    local_square = jnp.sum(valid_slot * local_center * local_center, axis=(0, 1))
    stats = jnp.stack([local_sum, local_square, jnp.full_like(local_sum, local_count)])
    stats = spread(stats, "fsdp", None, lax.axis_size("fsdp"))
    stats = spread(stats, "dp", None, lax.axis_size("dp")).reshape(-1, 3, stats.shape[-1])
    sums, squares, sizes = stats[:, 0], stats[:, 1], stats[:, 2]
    segment_total = jnp.sum(sizes, axis=0)
    batch_center = jnp.sum(sums, axis=0) / segment_total
    center = visual_rows - batch_center
    variance = (
        jnp.sum(squares + sizes * jnp.square(sums / sizes - batch_center), axis=0) / segment_total
    )
    inverse_spread = lax.rsqrt(variance + eps_batch)
    normed = center * inverse_spread
    embedded = (
        normed * full_batch_gain.astype(jnp.float32) + full_batch_shift.astype(jnp.float32)
    ).astype(jnp.bfloat16)
    joined = text_rows.astype(jnp.float32) + jnp.einsum(
        "drs,dsc->drc", onehot, embedded, preferred_element_type=jnp.float32
    )
    joined_low = joined.astype(jnp.bfloat16)
    packed = jnp.einsum(
        "drc,ce->dre", joined_low, full_attend, preferred_element_type=jnp.float32
    ).astype(jnp.bfloat16)
    attended, log_total = lax.map(attend_doc, (packed, padding_mask))
    projected = jnp.einsum("drc,ce->dre", attended, full_merge, preferred_element_type=jnp.float32)
    pre_one = joined + projected
    hidden_state = layer_norm(
        pre_one, full_first_gain.astype(jnp.float32), full_first_shift.astype(jnp.float32)
    )
    hidden_reduced_precision = hidden_state.astype(jnp.bfloat16)
    inner_hidden = jnp.einsum(
        "sjq,qy->sjy",
        hidden_reduced_precision,
        gathered_up_weight,
        preferred_element_type=jnp.float32,
    )
    gelu_activated = exact_gelu(inner_hidden).astype(jnp.bfloat16)
    residual_branch = jnp.einsum(
        "zya,av->zyv", gelu_activated, gathered_down_weight, preferred_element_type=jnp.float32
    )
    pre_two = hidden_state + residual_branch
    layer_output = layer_norm(
        pre_two, full_second_gain.astype(jnp.float32), full_second_shift.astype(jnp.float32)
    )
    visual_pullback = gathered_visual_weight
    back_batch_gain = full_batch_gain
    back_attend = full_attend
    back_merge = full_merge
    back_first_gain = full_first_gain
    up_pullback = gathered_up_weight
    down_pullback = gathered_down_weight
    back_second_gain = full_second_gain
    second_back = jax.vjp(
        layer_norm,
        pre_two,
        back_second_gain.astype(jnp.float32),
        full_second_shift.astype(jnp.float32),
    )[1]
    delta_two, second_gain_local, second_shift_local = second_back(cotangent.astype(jnp.float32))
    branch_gradient = delta_two.astype(jnp.bfloat16)
    down_local = jnp.einsum(
        "omt,oms->ts", gelu_activated, branch_gradient, preferred_element_type=jnp.float32
    )
    delta_activated = jnp.einsum(
        "ivj,hj->ivh", branch_gradient, down_pullback, preferred_element_type=jnp.float32
    )
    gelu_back = jax.vjp(exact_gelu, inner_hidden)[1]
    inner_gradient = gelu_back(delta_activated)[0].astype(jnp.bfloat16)
    up_local = jnp.einsum(
        "oih,oiu->hu", hidden_reduced_precision, inner_gradient, preferred_element_type=jnp.float32
    )
    delta_hidden = delta_two + jnp.einsum(
        "wmx,ix->wmi", inner_gradient, up_pullback, preferred_element_type=jnp.float32
    )
    first_back = jax.vjp(
        layer_norm,
        pre_one,
        back_first_gain.astype(jnp.float32),
        full_first_shift.astype(jnp.float32),
    )[1]
    delta_one, first_gain_local, first_shift_local = first_back(delta_hidden)
    delta_projected = delta_one.astype(jnp.bfloat16)
    merge_local = jnp.einsum(
        "drc,dre->ce", attended, delta_projected, preferred_element_type=jnp.float32
    )
    delta_attended = jnp.einsum(
        "dre,ce->drc", delta_projected, back_merge, preferred_element_type=jnp.float32
    ).astype(jnp.bfloat16)
    delta_packed = lax.map(attend_back, (packed, padding_mask, log_total, delta_attended))
    attend_local = jnp.einsum(
        "drc,dre->ce", joined_low, delta_packed, preferred_element_type=jnp.float32
    )
    delta_joined = delta_one + jnp.einsum(
        "dre,ce->drc", delta_packed, back_attend, preferred_element_type=jnp.float32
    )
    delta_embedded = jnp.einsum(
        "drs,drc->dsc",
        onehot_wide,
        delta_joined,
        precision=highest_precision,
        preferred_element_type=jnp.float32,
    )
    vectors = sum_all(
        jnp.stack(
            [
                jnp.sum(delta_embedded, axis=(0, 1)),
                jnp.sum(delta_embedded * normed, axis=(0, 1)),
                first_gain_local,
                first_shift_local,
                second_gain_local,
                second_shift_local,
            ]
        )
    )
    shift_total, gain_total = vectors[0], vectors[1]
    visual_delta_rows = (
        valid_slot
        * back_batch_gain.astype(jnp.float32)
        * inverse_spread
        * (delta_embedded - shift_total / segment_total - normed * gain_total / segment_total)
    ).astype(jnp.bfloat16)
    visual_local = jnp.einsum(
        "bli,blz->iz", pooled_segments, visual_delta_rows, preferred_element_type=jnp.float32
    )
    delta_pooled = (
        jnp.einsum(
            "zbl,wl->zbw", visual_delta_rows, visual_pullback, preferred_element_type=jnp.float32
        )
        / divisor
    )
    text_gradient = delta_joined + jnp.einsum(
        "drs,dsc->drc",
        onehot_wide,
        delta_pooled,
        precision=highest_precision,
        preferred_element_type=jnp.float32,
    )
    down_gradient = scatter_gradient(down_local)
    up_gradient = scatter_gradient(up_local)
    merge_gradient = scatter_gradient(merge_local)
    attend_gradient = scatter_gradient(attend_local)
    visual_gradient = scatter_gradient(visual_local)
    piece = features // lax.axis_size("fsdp")
    start = lax.axis_index("fsdp") * piece
    own = lax.dynamic_slice_in_dim(vectors, start, piece, 1)
    batch_shift_gradient, batch_gain_gradient = own[0], own[1]
    first_gain_gradient, first_shift_gradient = own[2], own[3]
    second_gain_gradient, second_shift_gradient = own[4], own[5]
    return (
        layer_output,
        text_gradient,
        visual_gradient,
        batch_gain_gradient,
        batch_shift_gradient,
        attend_gradient,
        merge_gradient,
        first_gain_gradient,
        first_shift_gradient,
        up_gradient,
        down_gradient,
        second_gain_gradient,
        second_shift_gradient,
    )


def solution(mesh):
    in_specs = (
        P(("dp", "fsdp"), None, None),
        P("fsdp", None),
        P("fsdp"),
        P("fsdp"),
        P("fsdp", None),
        P("fsdp", None),
        P("fsdp"),
        P("fsdp"),
        P("fsdp", None),
        P("fsdp", None),
        P("fsdp"),
        P("fsdp"),
        P(("dp", "fsdp")),
        P(("dp", "fsdp"), None),
        P(("dp", "fsdp"), None),
        P(("dp", "fsdp"), None, None),
    )
    out_specs = (
        P(("dp", "fsdp"), None, None),
        P(("dp", "fsdp"), None, None),
        P("fsdp", None),
        P("fsdp"),
        P("fsdp"),
        P("fsdp", None),
        P("fsdp", None),
        P("fsdp"),
        P("fsdp"),
        P("fsdp", None),
        P("fsdp", None),
        P("fsdp"),
        P("fsdp"),
    )
    return jax.shard_map(shards, mesh=mesh, in_specs=in_specs, out_specs=out_specs, check_vma=False)
```

```python
import functools

import jax
import jax.numpy as jnp
from jax import lax
from jax.experimental import pallas as pl
from jax.experimental.pallas import tpu as pltpu
from jax.sharding import PartitionSpec as P

HEADS = 12
SEGMAX = 128
low = jnp.bfloat16
wide = jnp.float32
eps_norm = 1e-05
eps_batch = 1e-05
masked_score = -1e30
highest_precision = lax.Precision.HIGHEST

NN = (((1,), (0,)), ((), ()))
NT = (((1,), (1,)), ((), ()))
TN = (((0,), (0,)), ((), ()))

tail_spread = 0.39 * 2**-0.5
tail_poly = [
    0.5 * value
    for value in (
        0.22003657898400666,
        0.21993814342134163,
        0.20469834418114297,
        0.1590209501745049,
        0.17253866336379592,
        -0.06413901990527864,
        0.25209925299909935,
        -0.21837884731666118,
        0.05418596701413587,
    )
]


def dot(left, right, dims=NN):
    return lax.dot_general(left, right, dims, preferred_element_type=wide)


def shape(dims, dtype=low):
    return jax.ShapeDtypeStruct(dims, dtype)


def call(kernel, name, grid, in_specs, out_specs, out_shape, scratch=(), aliases=None, cost=None):
    return pl.pallas_call(
        kernel,
        name=name,
        grid_spec=pltpu.PrefetchScalarGridSpec(
            num_scalar_prefetch=1,
            grid=grid,
            in_specs=in_specs,
            out_specs=out_specs,
            scratch_shapes=list(scratch),
        ),
        out_shape=out_shape,
        input_output_aliases=aliases or {},
        cost_estimate=cost,
        compiler_params=pltpu.CompilerParams(vmem_limit_bytes=56 * 2**20),
    )


def cost(flops, moved):
    return pl.CostEstimate(flops=int(flops), bytes_accessed=int(moved), transcendentals=0)


def pair_groups(size):
    return [[i, i + 1] for i in range(0, size, 2)]


def line_groups(size):
    return [list(range(0, size, 2)), list(range(1, size, 2))]


def spread(value, axis, groups, count):
    copies = jnp.broadcast_to(value[None], (count,) + value.shape)
    return lax.all_to_all(copies, axis, 0, 0, axis_index_groups=groups)


def swap(value, axis, bit):
    size = lax.axis_size(axis)
    return lax.ppermute(value, axis, [(i, i ^ bit) for i in range(size)])


def half_of(value, index):
    half = value.shape[-1] // 2
    return lax.dynamic_slice_in_dim(value, index * half, half, value.ndim - 1)


def gather_quick(mine):
    fsdp = lax.axis_size("fsdp")
    own = spread(mine, "fsdp", None, fsdp).reshape((fsdp * mine.shape[0],) + mine.shape[1:])
    return own, swap(own, "dp", 1)


def gather_bulk(mine):
    own = lax.all_gather(mine, "fsdp", axis=0, tiled=True)
    return own, swap(own, "dp", 1)


def join(own, other, core):
    return jnp.where(
        core == 0,
        jnp.concatenate([own, other], axis=-1),
        jnp.concatenate([other, own], axis=-1),
    )


def add_low(left, right):
    return (left.astype(wide) + right.astype(wide)).astype(low)


def finish(total, core):
    bit = 2
    while bit < lax.axis_size("dp"):
        total = add_low(total, swap(total, "dp", bit))
        bit *= 2
    return total, swap(total, "dp", 1)


def scatter_bulk(keep, give, core):
    chip = add_low(keep, swap(give, "dp", 1))
    return finish(lax.psum_scatter(chip, "fsdp", scatter_dimension=0, tiled=True), core)


def scatter_quick(keep, give, core):
    rows, half = keep.shape
    fsdp = lax.axis_size("fsdp")
    side = lax.axis_index("fsdp") % 2
    chip = add_low(keep, swap(give, "dp", 1)).reshape(fsdp // 2, 2, rows // fsdp, half)
    keep = lax.dynamic_index_in_dim(chip, side, 1, False)
    give = lax.dynamic_index_in_dim(chip, 1 - side, 1, False)
    pair = add_low(keep, swap(give, "fsdp", 1))
    parts = lax.all_to_all(pair, "fsdp", 0, 0, axis_index_groups=line_groups(fsdp))
    return finish(jnp.sum(parts.astype(wide), axis=0).astype(low), core)


def project_kernel(core_ref, x_ref, own_ref, other_ref, out_ref):
    @pl.when(pl.program_id(0) == 0)
    def _():
        out_ref[...] = dot(x_ref[...], own_ref[...]).astype(low)

    @pl.when(pl.program_id(0) == 1)
    def _():
        out_ref[...] = dot(x_ref[...], other_ref[...]).astype(low)


def project(x, own, other, core):
    rows, features = x.shape
    half = features // 2
    parts = own.shape[1] // half
    return call(
        project_kernel,
        "project",
        (2, parts),
        [
            pl.BlockSpec((rows, features), lambda s, j, c: (0, 0)),
            pl.BlockSpec((features, half), lambda s, j, c: (0, jnp.where(s == 0, j, parts - 1))),
            pl.BlockSpec((features, half), lambda s, j, c: (0, jnp.where(s == 1, j, 0))),
        ],
        pl.BlockSpec((rows, half), lambda s, j, c: (0, 2 * j + jnp.where(s == 0, c[0], 1 - c[0]))),
        shape((rows, 2 * own.shape[1])),
        cost=cost(4 * rows * features * own.shape[1], 2 * (rows * features + 2 * own.size * 3)),
    )(core, x, own, other)


def attend_kernel(core_ref, q_ref, k_ref, v_ref, mask_ref, out_ref, share_ref):
    queries, keys, values = q_ref[...], k_ref[...], v_ref[...]
    first = lax.broadcasted_iota(jnp.int32, queries.shape, 1) < queries.shape[1] // 2
    real = mask_ref[...] > 0
    mixed = []
    for head in range(2):
        mine = first if head == 0 else jnp.logical_not(first)
        scaled = jnp.where(mine, queries, jnp.zeros_like(queries)) * jnp.asarray(0.125, low)
        scores = jnp.where(real, dot(scaled, keys, NT), masked_score)
        raised = jnp.exp(scores - jnp.max(scores, axis=-1, keepdims=True))
        share = (raised * (1.0 / jnp.sum(raised, axis=-1, keepdims=True))).astype(low)
        share_ref[head] = share
        mixed.append(dot(share, values))
    out_ref[...] = jnp.where(first, mixed[0], mixed[1]).astype(low)


def column_spec(length, offset):
    return pl.BlockSpec((None, length, 128), lambda d, h, c: (d, 0, h + offset))


def attend(packed, mask, core):
    docs, length, columns = packed.shape
    pairs = columns // 3 // 128
    return call(
        attend_kernel,
        "attend",
        (docs, pairs),
        [
            column_spec(length, 0),
            column_spec(length, pairs),
            column_spec(length, 2 * pairs),
            pl.BlockSpec((None, 1, length), lambda d, h, c: (d, 0, 0)),
        ],
        [
            column_spec(length, 0),
            pl.BlockSpec((None, 2, length, length), lambda d, h, c: (d, h, 0, 0)),
        ],
        [
            shape((docs, length, columns // 3)),
            shape((docs, 2 * pairs, length, length)),
        ],
        cost=cost(docs * pairs * 8 * length * length * 256, docs * pairs * 4 * length * length),
    )(core, packed, packed, packed, mask[:, None, :])


def attend_back_kernel(core_ref, q_ref, k_ref, v_ref, share_ref, delta_ref, mixed_ref, out_ref):
    queries, keys, values, delta = q_ref[...], k_ref[...], v_ref[...], delta_ref[...]
    half = queries.shape[1] // 2
    first = lax.broadcasted_iota(jnp.int32, queries.shape, 1) < half
    product = delta.astype(wide) * mixed_ref[...].astype(wide)
    queries_t, delta_t = queries.T, delta.T
    for_queries, for_keys, for_values = [], [], []
    for head in range(2):
        mine = first if head == 0 else jnp.logical_not(first)
        delta_share = dot(jnp.where(mine, delta, jnp.zeros_like(delta)), values, NT)
        row = jnp.sum(jnp.where(mine, product, 0.0), axis=-1, keepdims=True)
        share = share_ref[head]
        delta_scores = (share.astype(wide) * (delta_share - row)).astype(low)
        for_queries.append(dot(delta_scores, keys))
        for_keys.append(dot(queries_t[half * head : half * (head + 1)], delta_scores))
        for_values.append(dot(delta_t[half * head : half * (head + 1)], share))
    out_ref[0] = (jnp.where(first, for_queries[0], for_queries[1]) * 0.125).astype(low)
    out_ref[1] = (jnp.concatenate(for_keys, 0) * 0.125).astype(low).T
    out_ref[2] = jnp.concatenate(for_values, 0).astype(low).T


def attend_back(packed, share, delta, mixed, core):
    docs, length, columns = packed.shape
    pairs = columns // 3 // 128
    return call(
        attend_back_kernel,
        "attend_back",
        (docs, pairs),
        [
            column_spec(length, 0),
            column_spec(length, pairs),
            column_spec(length, 2 * pairs),
            pl.BlockSpec((None, 2, length, length), lambda d, h, c: (d, h, 0, 0)),
            column_spec(length, 0),
            column_spec(length, 0),
        ],
        pl.BlockSpec((3, None, length, 128), lambda d, h, c: (0, d, 0, h)),
        shape((3, docs, length, columns // 3)),
        cost=cost(docs * pairs * 20 * length * length * 128, docs * pairs * 4 * length * length),
    )(core, packed, packed, packed, share, delta, mixed)


def gelu_parts(value):
    ratio = 1.0 / (1.0 + tail_spread * jnp.abs(value))
    poly = tail_poly[-1]
    for coefficient in tail_poly[-2::-1]:
        poly = poly * ratio + coefficient
    bell = jnp.exp(-0.5 * value * value)
    tail = poly * ratio * bell
    below = jnp.where(value < 0, tail, 1.0 - tail)
    return value * below, below + value * (bell * 0.3989422804014327)


def up_kernel(core_ref, x_ref, own_ref, other_ref, out_ref, slope_ref):
    def block(weight):
        value, slope = gelu_parts(dot(x_ref[...], weight))
        out_ref[...] = value.astype(low)
        slope_ref[...] = slope.astype(low)

    @pl.when(pl.program_id(0) == 0)
    def _():
        block(own_ref[...])

    @pl.when(pl.program_id(0) == 1)
    def _():
        block(other_ref[...])


def up(x, own, other, core, columns=512, rows=512):
    count, features = x.shape
    half = own.shape[1]
    steps = half // columns
    out = pl.BlockSpec(
        (rows, columns), lambda s, j, i, c: (i, j + steps * jnp.where(s == 0, c[0], 1 - c[0]))
    )
    return call(
        up_kernel,
        "up",
        (2, steps, count // rows),
        [
            pl.BlockSpec((rows, features), lambda s, j, i, c: (i, 0)),
            pl.BlockSpec((features, columns), lambda s, j, i, c: (0, jnp.where(s == 0, j, steps - 1))),
            pl.BlockSpec((features, columns), lambda s, j, i, c: (0, jnp.where(s == 1, j, 0))),
        ],
        [out, out],
        [shape((count, 2 * half))] * 2,
        cost=cost(4 * count * features * half, 4 * (features * half + 2 * count * half)),
    )(core, x, own, other)


def normalize(value):
    center = value - jnp.mean(value, axis=-1, keepdims=True)
    scale = lax.rsqrt(jnp.mean(center * center, axis=-1, keepdims=True) + eps_norm)
    return center * scale, scale


def normalize_back(scale, unit, delta):
    return scale * (
        delta
        - jnp.mean(delta, axis=-1, keepdims=True)
        - unit * jnp.mean(delta * unit, axis=-1, keepdims=True)
    )


def merge_kernel(core_ref, x_ref, joined_ref, weight_ref, vectors_ref, sum_ref, low_ref):
    total = joined_ref[...] + dot(x_ref[...], weight_ref[...])
    sum_ref[...] = total
    unit, _ = normalize(total)
    low_ref[...] = (unit * vectors_ref[0:1, :] + vectors_ref[1:2, :]).astype(low)


def merge(x, joined, weight, vectors, core, rows=256):
    count, features = x.shape
    block = pl.BlockSpec((rows, features), lambda i, c: (i, 0))
    return call(
        merge_kernel,
        "merge",
        (count // rows,),
        [
            block,
            block,
            pl.BlockSpec(weight.shape, lambda i, c: (0, 0)),
            pl.BlockSpec(vectors.shape, lambda i, c: (0, 0)),
        ],
        [block, block],
        [shape((count, features), wide), shape((count, features))],
        cost=cost(2 * count * features * features, 14 * count * features),
    )(core, x, joined, weight, vectors)


def fetch(own, other, target, sems, core):
    half = own.shape[1]
    mine = pl.multiple_of(core * half, 128)
    theirs = pl.multiple_of((1 - core) * half, 128)
    return (
        pltpu.make_async_copy(own, target.at[:, pl.ds(mine, half)], sems.at[0]),
        pltpu.make_async_copy(other, target.at[:, pl.ds(theirs, half)], sems.at[1]),
    )


def down_kernel(
    core_ref,
    x_ref,
    sum_ref,
    cotangent_ref,
    vectors_ref,
    own_ref,
    other_ref,
    out_ref,
    delta_ref,
    low_ref,
    sums_ref,
    weight,
    sems,
):
    @pl.when(pl.program_id(0) == 0)
    def _():
        copies = fetch(own_ref, other_ref, weight, sems, core_ref[0])
        for copy in copies:
            copy.start()
        sums_ref[...] = jnp.zeros_like(sums_ref)
        for copy in copies:
            copy.wait()

    unit, _ = normalize(sum_ref[...])
    hidden = unit * vectors_ref[0:1, :] + vectors_ref[1:2, :]
    unit, scale = normalize(hidden + dot(x_ref[...], weight[...]))
    out_ref[...] = unit * vectors_ref[2:3, :] + vectors_ref[3:4, :]
    given = cotangent_ref[...].astype(wide)
    delta = normalize_back(scale, unit, given * vectors_ref[2:3, :])
    delta_ref[...] = delta
    low_ref[...] = delta.astype(low)
    sums_ref[0:1, :] += jnp.sum(given * unit, axis=0, keepdims=True)
    sums_ref[1:2, :] += jnp.sum(given, axis=0, keepdims=True)


def down(x, total, cotangent, vectors, own, other, core, rows=256):
    count, hidden = x.shape
    features = total.shape[1]
    block = pl.BlockSpec((rows, features), lambda i, c: (i, 0))
    return call(
        down_kernel,
        "down",
        (count // rows,),
        [
            pl.BlockSpec((rows, hidden), lambda i, c: (i, 0)),
            block,
            block,
            pl.BlockSpec(vectors.shape, lambda i, c: (0, 0)),
            pl.BlockSpec(memory_space=pl.ANY),
            pl.BlockSpec(memory_space=pl.ANY),
        ],
        [block, block, block, pl.BlockSpec((8, features), lambda i, c: (0, 0))],
        [
            shape((count, features), wide),
            shape((count, features), wide),
            shape((count, features)),
            shape((8, features), wide),
        ],
        [pltpu.VMEM((hidden, features), low), pltpu.SemaphoreType.DMA((2,))],
        cost=cost(2 * count * features * hidden, 12 * count * features + 4 * count * hidden),
    )(core, x, total, cotangent, vectors, own, other)


def inner_kernel(
    core_ref,
    low_ref,
    delta_ref,
    slope_ref,
    sum_ref,
    vectors_ref,
    merge_ref,
    down_own_ref,
    down_other_ref,
    up_own_ref,
    up_other_ref,
    inner_ref,
    one_ref,
    one_low_ref,
    mixed_ref,
    sums_ref,
    down_weight,
    up_weight,
    sems,
):
    core = core_ref[0]

    def copies():
        return (
            *fetch(down_own_ref, down_other_ref, down_weight, sems.at[0], core),
            *fetch(up_own_ref, up_other_ref, up_weight, sems.at[1], core),
        )

    @pl.when(pl.program_id(0) == 0)
    def _():
        started = copies()
        for copy in started:
            copy.start()
        sums_ref[...] = jnp.zeros_like(sums_ref)
        for copy in started:
            copy.wait()

    inner = (dot(low_ref[...], down_weight[...], NT) * slope_ref[...].astype(wide)).astype(low)
    inner_ref[...] = inner
    delta = delta_ref[...] + dot(inner, up_weight[...], NT)
    unit, scale = normalize(sum_ref[...])
    one = normalize_back(scale, unit, delta * vectors_ref[0:1, :])
    one_ref[...] = one
    one_low = one.astype(low)
    one_low_ref[...] = one_low
    mixed_ref[...] = dot(one_low, merge_ref[...], NT).astype(low)
    sums_ref[0:1, :] += jnp.sum(delta * unit, axis=0, keepdims=True)
    sums_ref[1:2, :] += jnp.sum(delta, axis=0, keepdims=True)


def inner_back(branch, delta, slope, total, vectors, weight, downs, ups, core, rows=256):
    count, hidden = slope.shape
    features = total.shape[1]
    block = pl.BlockSpec((rows, features), lambda i, c: (i, 0))
    tall = pl.BlockSpec((rows, hidden), lambda i, c: (i, 0))
    anywhere = pl.BlockSpec(memory_space=pl.ANY)
    return call(
        inner_kernel,
        "inner_back",
        (count // rows,),
        [
            block,
            block,
            tall,
            block,
            pl.BlockSpec(vectors.shape, lambda i, c: (0, 0)),
            pl.BlockSpec(weight.shape, lambda i, c: (0, 0)),
            anywhere,
            anywhere,
            anywhere,
            anywhere,
        ],
        [tall, block, block, block, pl.BlockSpec((8, features), lambda i, c: (0, 0))],
        [
            shape((count, hidden)),
            shape((count, features), wide),
            shape((count, features)),
            shape((count, features)),
            shape((8, features), wide),
        ],
        [
            pltpu.VMEM((hidden, features), low),
            pltpu.VMEM((features, hidden), low),
            pltpu.SemaphoreType.DMA((2, 2)),
        ],
        cost=cost(4 * count * features * hidden, 16 * count * features + 8 * count * hidden),
    )(core, branch, delta, slope, total, vectors, weight, *downs, *ups)


def columns_kernel(core_ref, left_ref, own_ref, other_ref, keep_ref, give_ref):
    half = own_ref.shape[-1]
    both = jnp.concatenate([own_ref[...], other_ref[...]], axis=1)
    total = dot(left_ref[...], both, TN)
    keep_ref[...] = total[:, :half].astype(low)
    give_ref[...] = total[:, half:].astype(low)


def weight_columns(left, right, core, rows=768):
    count, height = left.shape
    parts, _, width = right.shape
    half = width // 2
    steps = height // rows
    out = pl.BlockSpec((rows, half), lambda p, j, c: (j, p))
    return call(
        columns_kernel,
        "weight_columns",
        (parts, steps),
        [
            pl.BlockSpec((count, rows), lambda p, j, c: (0, j)),
            pl.BlockSpec((None, count, half), lambda p, j, c: (p, 0, c[0])),
            pl.BlockSpec((None, count, half), lambda p, j, c: (p, 0, 1 - c[0])),
        ],
        [out, out],
        [shape((height, parts * half))] * 2,
        cost=cost(
            2 * parts * count * height * width, 2 * (count * height + parts * width * (count + height))
        ),
    )(core, left, right, right)


def wide_kernel(core_ref, left_ref, right_ref, keep_ref, give_ref):
    total = dot(left_ref[...], right_ref[...], TN).astype(low)

    @pl.when(pl.program_id(0) == 0)
    def _():
        give_ref[...] = total

    @pl.when(pl.program_id(0) == 1)
    def _():
        keep_ref[...] = total


def weight_wide(left, right, core, columns=768):
    count, height = left.shape
    steps = right.shape[1] // 2 // columns
    return call(
        wide_kernel,
        "weight_wide",
        (2, steps),
        [
            pl.BlockSpec((count, height), lambda s, j, c: (0, 0)),
            pl.BlockSpec(
                (count, columns), lambda s, j, c: (0, j + steps * jnp.where(s == 0, 1 - c[0], c[0]))
            ),
        ],
        [
            pl.BlockSpec((height, columns), lambda s, j, c: (0, jnp.where(s == 1, j, 0))),
            pl.BlockSpec((height, columns), lambda s, j, c: (0, jnp.where(s == 0, j, steps - 1))),
        ],
        [shape((height, right.shape[1] // 2))] * 2,
        cost=cost(2 * count * height * right.shape[1], 2 * (count + height) * right.shape[1]),
    )(core, left, right)


def joined_kernel(core_ref, one_ref, left_ref, right_ref, own_ref, other_ref, out_ref, total):
    part = pl.program_id(1)

    @pl.when(part == 0)
    def _():
        total[...] = one_ref[...]

    both = jnp.concatenate([left_ref[...], right_ref[...]], axis=1)
    weight = jnp.concatenate([own_ref[...], other_ref[...]], axis=1)
    total[...] += dot(both, weight, NT)

    @pl.when(part == pl.num_programs(1) - 1)
    def _():
        out_ref[...] = total[...]


def joined_back(one, packed, own, other, core, rows=1024):
    count, features = one.shape
    parts = packed.shape[0]
    half = features // 2
    block = pl.BlockSpec((rows, features), lambda i, p, c: (i, 0))
    weight = pl.BlockSpec((features, half), lambda i, p, c: (0, p))
    return call(
        joined_kernel,
        "joined_back",
        (count // rows, parts),
        [
            block,
            pl.BlockSpec((None, rows, half), lambda i, p, c: (p, i, c[0])),
            pl.BlockSpec((None, rows, half), lambda i, p, c: (p, i, 1 - c[0])),
            weight,
            weight,
        ],
        block,
        shape((count, features), wide),
        [pltpu.VMEM((rows, features), wide)],
        cost=cost(2 * parts * count * features * features, 14 * count * features),
    )(core, one, packed, packed, own, other)


def shards(
    text_rows,
    visual_matrix,
    batch_gain,
    batch_shift,
    attend_weight,
    merge_weight,
    first_gain,
    first_shift,
    up_matrix,
    down_matrix,
    second_gain,
    second_shift,
    segment_counts,
    segment_ids,
    padding_mask,
    cotangent,
):
    docs, length, features = text_rows.shape
    count = docs * length
    half = features // 2
    dp, fsdp = lax.axis_size("dp"), lax.axis_size("fsdp")
    core = lax.axis_index("dp") % 2
    which = core.reshape(1).astype(jnp.int32)
    piece = features // fsdp

    small = jnp.stack(
        [first_gain, first_shift, second_gain, second_shift, batch_gain, batch_shift]
    )
    visual_own, visual_other = gather_quick(half_of(visual_matrix, core))
    small = spread(small, "fsdp", None, fsdp).transpose(1, 0, 2).reshape(6, features)
    vectors = jnp.pad(small.astype(wide), ((0, 2), (0, 0)))
    full_batch_gain, full_batch_shift = vectors[4], vectors[5]
    mine = half_of(attend_weight.reshape(piece, 3, features), core).reshape(piece, 3 * half)
    attend_own, attend_other = gather_quick(mine)
    merge_own, merge_other = gather_quick(half_of(merge_weight, core))
    ups = gather_bulk(half_of(up_matrix, core))
    downs = gather_bulk(half_of(down_matrix, core))
    full_visual = join(visual_own, visual_other, core)
    full_merge = join(merge_own, merge_other, core)

    slot_index = jnp.arange(SEGMAX)
    matches = segment_ids[:, :, None] == slot_index[None, None, :]
    onehot = matches.astype(low)
    onehot_wide = matches.astype(wide)
    divisor = jnp.maximum(jnp.sum(onehot_wide, axis=1), 1.0)[..., None]
    pooled_segments = (
        jnp.einsum("drs,drc->dsc", onehot, text_rows, preferred_element_type=wide) / divisor
    ).astype(low)
    visual_rows = jnp.einsum(
        "bil,ly->biy", pooled_segments, full_visual, preferred_element_type=wide
    )
    valid_slot = (slot_index[None, :] < segment_counts[:, None]).astype(wide)[..., None]
    local_count = jnp.sum(segment_counts).astype(wide)
    local_sum = jnp.sum(valid_slot * visual_rows, axis=(0, 1))
    local_center = visual_rows - local_sum / local_count
    local_square = jnp.sum(valid_slot * local_center * local_center, axis=(0, 1))
    stats = jnp.stack([local_sum, local_square, jnp.full_like(local_sum, local_count)])
    stats = spread(stats, "fsdp", None, fsdp)
    stats = spread(stats, "dp", None, dp).reshape(-1, 3, features)
    sums, squares, sizes = stats[:, 0], stats[:, 1], stats[:, 2]
    segment_total = jnp.sum(sizes, axis=0)
    batch_center = jnp.sum(sums, axis=0) / segment_total
    center = visual_rows - batch_center
    variance = (
        jnp.sum(squares + sizes * jnp.square(sums / sizes - batch_center), axis=0) / segment_total
    )
    inverse_spread = lax.rsqrt(variance + eps_batch)
    normed = center * inverse_spread
    embedded = (normed * full_batch_gain + full_batch_shift).astype(low)
    joined = text_rows.astype(wide) + jnp.einsum(
        "drs,dsc->drc", onehot, embedded, preferred_element_type=wide
    )
    joined = joined.reshape(count, features)
    joined_low = joined.astype(low)

    packed = project(joined_low, attend_own, attend_other, which).reshape(docs, length, -1)
    attended, share = attend(packed, padding_mask, which)
    flat_attended = attended.reshape(count, features)
    total_one, hidden_low = merge(flat_attended, joined, full_merge, vectors, which)
    activated, slope = up(hidden_low, *ups, which)
    layer_output, delta_two, branch_low, sums_two = down(
        activated, total_one, cotangent.reshape(count, features), vectors, *downs, which
    )

    down_halves = weight_columns(activated, branch_low[None], which)
    down_shard = scatter_bulk(*down_halves, core)
    delta_inner, delta_one, one_low, delta_attended, sums_one = inner_back(
        branch_low, delta_two, slope, total_one, vectors, full_merge, downs, ups, which
    )
    up_halves = weight_wide(hidden_low, delta_inner, which)
    up_shard = scatter_bulk(*up_halves, core)
    merge_halves = weight_columns(flat_attended, one_low[None], which)
    merge_shard = scatter_quick(*merge_halves, core)
    delta_packed = attend_back(
        packed, share, delta_attended.reshape(docs, length, features), attended, which
    ).reshape(3, count, features)
    attend_halves = weight_columns(joined_low, delta_packed, which)
    attend_shard = scatter_quick(*attend_halves, core)
    delta_joined = joined_back(delta_one, delta_packed, attend_own, attend_other, which)
    delta_joined = delta_joined.reshape(docs, length, features)
    delta_embedded = jnp.einsum(
        "drs,drc->dsc",
        onehot_wide,
        delta_joined,
        precision=highest_precision,
        preferred_element_type=wide,
    )
    sums = jnp.stack(
        [
            sums_one[0],
            sums_one[1],
            sums_two[0],
            sums_two[1],
            jnp.sum(delta_embedded * normed, axis=(0, 1)),
            jnp.sum(delta_embedded, axis=(0, 1)),
        ]
    )
    sums = jnp.sum(spread(sums, "fsdp", None, fsdp), axis=0)
    sums = jnp.sum(spread(sums, "dp", None, dp), axis=0)
    gain_total, shift_total = sums[4], sums[5]
    visual_delta_rows = (
        valid_slot
        * full_batch_gain
        * inverse_spread
        * (delta_embedded - shift_total / segment_total - normed * gain_total / segment_total)
    ).astype(low)
    visual_local = jnp.einsum(
        "bli,blz->iz", pooled_segments, visual_delta_rows, preferred_element_type=wide
    ).astype(low)
    visual_shard = scatter_quick(half_of(visual_local, core), half_of(visual_local, 1 - core), core)
    delta_pooled = (
        jnp.einsum("zbl,wl->zbw", visual_delta_rows, full_visual, preferred_element_type=wide)
        / divisor
    )
    text_gradient = delta_joined + jnp.einsum(
        "drs,dsc->drc",
        onehot_wide,
        delta_pooled,
        precision=highest_precision,
        preferred_element_type=wide,
    )

    own = lax.dynamic_slice_in_dim(sums, lax.axis_index("fsdp") * piece, piece, 1)
    attend_gradient = join(
        attend_shard[0].reshape(piece, 3, half), attend_shard[1].reshape(piece, 3, half), core
    ).reshape(piece, 3 * features)
    return (
        layer_output.reshape(docs, length, features),
        text_gradient,
        join(*visual_shard, core).astype(wide),
        own[4],
        own[5],
        attend_gradient.astype(wide),
        join(*merge_shard, core).astype(wide),
        own[0],
        own[1],
        join(*up_shard, core).astype(wide),
        join(*down_shard, core).astype(wide),
        own[2],
        own[3],
    )


def solution(mesh):
    in_specs = (
        P(("dp", "fsdp"), None, None),
        P("fsdp", None),
        P("fsdp"),
        P("fsdp"),
        P("fsdp", None),
        P("fsdp", None),
        P("fsdp"),
        P("fsdp"),
        P("fsdp", None),
        P("fsdp", None),
        P("fsdp"),
        P("fsdp"),
        P(("dp", "fsdp")),
        P(("dp", "fsdp"), None),
        P(("dp", "fsdp"), None),
        P(("dp", "fsdp"), None, None),
    )
    out_specs = (
        P(("dp", "fsdp"), None, None),
        P(("dp", "fsdp"), None, None),
        P("fsdp", None),
        P("fsdp"),
        P("fsdp"),
        P("fsdp", None),
        P("fsdp", None),
        P("fsdp"),
        P("fsdp"),
        P("fsdp", None),
        P("fsdp", None),
        P("fsdp"),
        P("fsdp"),
    )
    return jax.shard_map(shards, mesh=mesh, in_specs=in_specs, out_specs=out_specs, check_vma=False)
```

```python
import functools

import jax
import jax.numpy as jnp
from jax import lax
from jax.experimental import pallas as pl
from jax.experimental.pallas import tpu as pltpu
from jax.sharding import PartitionSpec as P

HEADS = 12
SEGMAX = 128
low = jnp.bfloat16
wide = jnp.float32
eps_norm = 1e-05
eps_batch = 1e-05
masked_score = -1e30
highest_precision = lax.Precision.HIGHEST

NN = (((1,), (0,)), ((), ()))
NT = (((1,), (1,)), ((), ()))
TN = (((0,), (0,)), ((), ()))

tail_spread = 0.39 * 2**-0.5
tail_poly = [
    0.5 * value
    for value in (
        0.22003657898400666,
        0.21993814342134163,
        0.20469834418114297,
        0.1590209501745049,
        0.17253866336379592,
        -0.06413901990527864,
        0.25209925299909935,
        -0.21837884731666118,
        0.05418596701413587,
    )
]


def dot(left, right, dims=NN):
    return lax.dot_general(left, right, dims, preferred_element_type=wide)


def shape(dims, dtype=low):
    return jax.ShapeDtypeStruct(dims, dtype)


def call(kernel, name, grid, in_specs, out_specs, out_shape, scratch=(), aliases=None):
    return pl.pallas_call(
        kernel,
        name=name,
        grid_spec=pltpu.PrefetchScalarGridSpec(
            num_scalar_prefetch=1,
            grid=grid,
            in_specs=in_specs,
            out_specs=out_specs,
            scratch_shapes=list(scratch),
        ),
        out_shape=out_shape,
        input_output_aliases=aliases or {},
        compiler_params=pltpu.CompilerParams(vmem_limit_bytes=56 * 2**20),
    )


def pair_groups(size):
    return [[i, i + 1] for i in range(0, size, 2)]


def line_groups(size):
    return [list(range(0, size, 2)), list(range(1, size, 2))]


def spread(value, axis, groups, count):
    copies = jnp.broadcast_to(value[None], (count,) + value.shape)
    return lax.all_to_all(copies, axis, 0, 0, axis_index_groups=groups)


def swap(value, axis, bit):
    size = lax.axis_size(axis)
    return lax.ppermute(value, axis, [(i, i ^ bit) for i in range(size)])


def half_of(value, index):
    half = value.shape[-1] // 2
    return lax.dynamic_slice_in_dim(value, index * half, half, value.ndim - 1)


def after(value, *others):
    return lax.optimization_barrier((value, *others))[0]


def gather_line(mine):
    line = lax.axis_index("fsdp") // 2
    around = [mine] + [
        lax.ppermute(mine, "fsdp", [(i, (i + 2 * step) % 8) for i in range(8)]) for step in (1, 2, 3)
    ]
    column = jnp.zeros((4,) + mine.shape, mine.dtype)
    for step in range(4):
        column = lax.dynamic_update_index_in_dim(column, around[step], (line - step) % 4, 0)
    return column


def gather_side(column):
    side = lax.axis_index("fsdp") % 2
    beside = swap(column, "fsdp", 1)
    own = jnp.where(
        side == 0, jnp.stack([column, beside], axis=1), jnp.stack([beside, column], axis=1)
    )
    return own.reshape(-1, column.shape[-1])


def gather_bulk(mine):
    return lax.all_gather(mine, "fsdp", axis=0, tiled=True)


def join(own, other, core):
    return jnp.where(
        core == 0,
        jnp.concatenate([own, other], axis=-1),
        jnp.concatenate([other, own], axis=-1),
    )


def add_low(left, right):
    return (left.astype(wide) + right.astype(wide)).astype(low)


def finish(total, core):
    bit = 2
    while bit < lax.axis_size("dp"):
        total = add_low(total, swap(total, "dp", bit))
        bit *= 2
    return total, swap(total, "dp", 1)


def scatter_small(keep, give, core):
    rows, half = keep.shape
    fsdp = lax.axis_size("fsdp")
    chip = add_low(keep, swap(give, "dp", 1)).reshape(fsdp, rows // fsdp, half)
    parts = lax.all_to_all(chip, "fsdp", 0, 0)
    return finish(jnp.sum(parts.astype(wide), axis=0).astype(low), core)


def scatter_begin(chip):
    rows, half = chip.shape
    fsdp = lax.axis_size("fsdp")
    side = lax.axis_index("fsdp") % 2
    chip = chip.reshape(fsdp // 2, 2, rows // fsdp, half)
    keep = lax.dynamic_index_in_dim(chip, side, 1, False)
    return keep, lax.dynamic_index_in_dim(chip, 1 - side, 1, False)


def scatter_end(keep, given, core):
    lines = keep.shape[0]
    line = lax.axis_index("fsdp") // 2
    pair = add_low(keep, given)
    total = lax.dynamic_index_in_dim(pair, line, 0, False).astype(wide)
    for step in range(1, lines):
        away = lax.dynamic_index_in_dim(pair, (line + step) % lines, 0, False)
        away = lax.ppermute(
            away, "fsdp", [(i, (i + 2 * step) % (2 * lines)) for i in range(2 * lines)]
        )
        total = total + away.astype(wide)
    return finish(total.astype(low), core)


def sum_all(value):
    for axis in ("dp", "fsdp"):
        bit = 1
        while bit < lax.axis_size(axis):
            value = value + swap(value, axis, bit)
            bit *= 2
    return value


def project_kernel(core_ref, x_ref, own_ref, other_ref, out_ref):
    half = own_ref.shape[1]
    both = jnp.concatenate([own_ref[...], other_ref[...]], axis=1)
    total = dot(x_ref[...], both).astype(low)
    out_ref[:, pl.ds(pl.multiple_of(core_ref[0] * half, 128), half)] = total[:, :half]
    out_ref[:, pl.ds(pl.multiple_of((1 - core_ref[0]) * half, 128), half)] = total[:, half:]


def project(x, own, other, core, rows=512):
    count, features = x.shape
    half = features // 2
    weight = pl.BlockSpec((features, half), lambda j, i, c: (0, j))
    return call(
        project_kernel,
        "project",
        (3, count // rows),
        [pl.BlockSpec((rows, features), lambda j, i, c: (i, 0)), weight, weight],
        pl.BlockSpec((rows, features), lambda j, i, c: (i, j)),
        shape((count, 3 * features)),
    )(core, x, own, other)


def attend_kernel(core_ref, q_ref, k_ref, v_ref, mask_ref, out_ref, share_ref):
    queries, keys, values = q_ref[...], k_ref[...], v_ref[...]
    first = lax.broadcasted_iota(jnp.int32, queries.shape, 1) < queries.shape[1] // 2
    real = mask_ref[...] > 0
    mixed = []
    for head in range(2):
        mine = first if head == 0 else jnp.logical_not(first)
        scaled = jnp.where(mine, queries, jnp.zeros_like(queries)) * jnp.asarray(0.125, low)
        scores = jnp.where(real, dot(scaled, keys, NT), masked_score)
        raised = jnp.exp(scores - jnp.max(scores, axis=-1, keepdims=True))
        share = (raised * (1.0 / jnp.sum(raised, axis=-1, keepdims=True))).astype(low)
        share_ref[head] = share
        mixed.append(dot(share, values))
    out_ref[...] = jnp.where(first, mixed[0], mixed[1]).astype(low)


def column_spec(length, offset):
    return pl.BlockSpec((None, length, 128), lambda d, h, c: (d, 0, h + offset))


def attend(packed, mask, core):
    docs, length, columns = packed.shape
    pairs = columns // 3 // 128
    return call(
        attend_kernel,
        "attend",
        (docs, pairs),
        [
            column_spec(length, 0),
            column_spec(length, pairs),
            column_spec(length, 2 * pairs),
            pl.BlockSpec((None, 1, length), lambda d, h, c: (d, 0, 0)),
        ],
        [
            column_spec(length, 0),
            pl.BlockSpec((None, 2, length, length), lambda d, h, c: (d, h, 0, 0)),
        ],
        [
            shape((docs, length, columns // 3)),
            shape((docs, 2 * pairs, length, length)),
        ],
    )(core, packed, packed, packed, mask[:, None, :])


def attend_back_kernel(core_ref, q_ref, k_ref, v_ref, share_ref, delta_ref, mixed_ref, out_ref):
    queries, keys, values, delta = q_ref[...], k_ref[...], v_ref[...], delta_ref[...]
    half = queries.shape[1] // 2
    first = lax.broadcasted_iota(jnp.int32, queries.shape, 1) < half
    product = delta.astype(wide) * mixed_ref[...].astype(wide)
    queries_t, delta_t = queries.T, delta.T
    for_queries, for_keys, for_values = [], [], []
    for head in range(2):
        mine = first if head == 0 else jnp.logical_not(first)
        delta_share = dot(jnp.where(mine, delta, jnp.zeros_like(delta)), values, NT)
        row = jnp.sum(jnp.where(mine, product, 0.0), axis=-1, keepdims=True)
        share = share_ref[head]
        delta_scores = (share.astype(wide) * (delta_share - row)).astype(low)
        for_queries.append(dot(delta_scores, keys))
        for_keys.append(dot(queries_t[half * head : half * (head + 1)], delta_scores))
        for_values.append(dot(delta_t[half * head : half * (head + 1)], share))
    out_ref[0] = (jnp.where(first, for_queries[0], for_queries[1]) * 0.125).astype(low)
    out_ref[1] = (jnp.concatenate(for_keys, 0) * 0.125).astype(low).T
    out_ref[2] = jnp.concatenate(for_values, 0).astype(low).T


def attend_back(packed, share, delta, mixed, core):
    docs, length, columns = packed.shape
    pairs = columns // 3 // 128
    return call(
        attend_back_kernel,
        "attend_back",
        (docs, pairs),
        [
            column_spec(length, 0),
            column_spec(length, pairs),
            column_spec(length, 2 * pairs),
            pl.BlockSpec((None, 2, length, length), lambda d, h, c: (d, h, 0, 0)),
            column_spec(length, 0),
            column_spec(length, 0),
        ],
        pl.BlockSpec((3, None, length, 128), lambda d, h, c: (0, d, 0, h)),
        shape((3, docs, length, columns // 3)),
    )(core, packed, packed, packed, share, delta, mixed)


def gelu_parts(value):
    ratio = 1.0 / (1.0 + tail_spread * jnp.abs(value))
    poly = tail_poly[-1]
    for coefficient in tail_poly[-2::-1]:
        poly = poly * ratio + coefficient
    bell = jnp.exp(-0.5 * value * value)
    tail = poly * ratio * bell
    below = jnp.where(value < 0, tail, 1.0 - tail)
    return value * below, below + value * (bell * 0.3989422804014327)


def up_kernel(core_ref, x_ref, own_ref, other_ref, out_ref, slope_ref):
    def block(weight):
        value, slope = gelu_parts(dot(x_ref[...], weight))
        out_ref[...] = value.astype(low)
        slope_ref[...] = slope.astype(low)

    @pl.when(pl.program_id(0) == 0)
    def _():
        block(own_ref[...])

    @pl.when(pl.program_id(0) == 1)
    def _():
        block(other_ref[...])


def up(x, own, other, core, columns=512, rows=512):
    count, features = x.shape
    half = own.shape[1]
    steps = half // columns
    out = pl.BlockSpec(
        (rows, columns), lambda s, j, i, c: (i, j + steps * jnp.where(s == 0, c[0], 1 - c[0]))
    )
    return call(
        up_kernel,
        "up",
        (2, steps, count // rows),
        [
            pl.BlockSpec((rows, features), lambda s, j, i, c: (i, 0)),
            pl.BlockSpec((features, columns), lambda s, j, i, c: (0, jnp.where(s == 0, j, steps - 1))),
            pl.BlockSpec((features, columns), lambda s, j, i, c: (0, jnp.where(s == 1, j, 0))),
        ],
        [out, out],
        [shape((count, 2 * half))] * 2,
    )(core, x, own, other)


def normalize(value):
    center = value - jnp.mean(value, axis=-1, keepdims=True)
    scale = lax.rsqrt(jnp.mean(center * center, axis=-1, keepdims=True) + eps_norm)
    return center * scale, scale


def normalize_back(scale, unit, delta):
    return scale * (
        delta
        - jnp.mean(delta, axis=-1, keepdims=True)
        - unit * jnp.mean(delta * unit, axis=-1, keepdims=True)
    )


def fetch(own, other, target, sems, core, start=0):
    half = target.shape[1] // 2
    own, other = own.at[:, pl.ds(start, half)], other.at[:, pl.ds(start, half)]
    mine = pl.multiple_of(core * half, 128)
    theirs = pl.multiple_of((1 - core) * half, 128)
    return (
        pltpu.make_async_copy(own, target.at[:, pl.ds(mine, half)], sems.at[0]),
        pltpu.make_async_copy(other, target.at[:, pl.ds(theirs, half)], sems.at[1]),
    )


def merge_kernel(
    core_ref, x_ref, joined_ref, vectors_ref, own_ref, other_ref, sum_ref, low_ref, weight, sems
):
    @pl.when(pl.program_id(0) == 0)
    def _():
        half = weight.shape[1] // 2
        copies = fetch(own_ref, other_ref, weight, sems, core_ref[0], 3 * half)
        for copy in copies:
            copy.start()
        for copy in copies:
            copy.wait()

    total = joined_ref[...] + dot(x_ref[...], weight[...])
    sum_ref[...] = total
    unit, _ = normalize(total)
    low_ref[...] = (unit * vectors_ref[0:1, :] + vectors_ref[1:2, :]).astype(low)


def merge(x, joined, vectors, own, other, core, rows=256):
    count, features = x.shape
    block = pl.BlockSpec((rows, features), lambda i, c: (i, 0))
    return call(
        merge_kernel,
        "merge",
        (count // rows,),
        [
            block,
            block,
            pl.BlockSpec(vectors.shape, lambda i, c: (0, 0)),
            pl.BlockSpec(memory_space=pl.ANY),
            pl.BlockSpec(memory_space=pl.ANY),
        ],
        [block, block],
        [shape((count, features), wide), shape((count, features))],
        [pltpu.VMEM((features, features), low), pltpu.SemaphoreType.DMA((2,))],
    )(core, x, joined, vectors, own, other)


def down_kernel(
    core_ref,
    x_ref,
    sum_ref,
    cotangent_ref,
    vectors_ref,
    own_ref,
    other_ref,
    out_ref,
    delta_ref,
    low_ref,
    sums_ref,
    weight,
    sems,
):
    @pl.when(pl.program_id(0) == 0)
    def _():
        copies = fetch(own_ref, other_ref, weight, sems, core_ref[0])
        for copy in copies:
            copy.start()
        sums_ref[...] = jnp.zeros_like(sums_ref)
        for copy in copies:
            copy.wait()

    unit, _ = normalize(sum_ref[...])
    hidden = unit * vectors_ref[0:1, :] + vectors_ref[1:2, :]
    unit, scale = normalize(hidden + dot(x_ref[...], weight[...]))
    out_ref[...] = unit * vectors_ref[2:3, :] + vectors_ref[3:4, :]
    given = cotangent_ref[...].astype(wide)
    delta = normalize_back(scale, unit, given * vectors_ref[2:3, :])
    delta_ref[...] = delta
    low_ref[...] = delta.astype(low)
    sums_ref[0:1, :] += jnp.sum(given * unit, axis=0, keepdims=True)
    sums_ref[1:2, :] += jnp.sum(given, axis=0, keepdims=True)


def down(x, total, cotangent, vectors, own, other, core, rows=256):
    count, hidden = x.shape
    features = total.shape[1]
    block = pl.BlockSpec((rows, features), lambda i, c: (i, 0))
    return call(
        down_kernel,
        "down",
        (count // rows,),
        [
            pl.BlockSpec((rows, hidden), lambda i, c: (i, 0)),
            block,
            block,
            pl.BlockSpec(vectors.shape, lambda i, c: (0, 0)),
            pl.BlockSpec(memory_space=pl.ANY),
            pl.BlockSpec(memory_space=pl.ANY),
        ],
        [block, block, block, pl.BlockSpec((8, features), lambda i, c: (0, 0))],
        [
            shape((count, features), wide),
            shape((count, features), wide),
            shape((count, features)),
            shape((8, features), wide),
        ],
        [pltpu.VMEM((hidden, features), low), pltpu.SemaphoreType.DMA((2,))],
    )(core, x, total, cotangent, vectors, own, other)


def inner_kernel(
    core_ref,
    low_ref,
    delta_ref,
    slope_ref,
    sum_ref,
    vectors_ref,
    merge_own_ref,
    merge_other_ref,
    down_own_ref,
    down_other_ref,
    up_own_ref,
    up_other_ref,
    inner_ref,
    one_ref,
    one_low_ref,
    mixed_ref,
    sums_ref,
    down_weight,
    up_weight,
    merge_weight,
    sems,
):
    core = core_ref[0]

    def copies():
        return (
            *fetch(down_own_ref, down_other_ref, down_weight, sems.at[0], core),
            *fetch(up_own_ref, up_other_ref, up_weight, sems.at[1], core),
            *fetch(
                merge_own_ref,
                merge_other_ref,
                merge_weight,
                sems.at[2],
                core,
                3 * merge_weight.shape[1] // 2,
            ),
        )

    @pl.when(pl.program_id(0) == 0)
    def _():
        started = copies()
        for copy in started:
            copy.start()
        sums_ref[...] = jnp.zeros_like(sums_ref)
        for copy in started:
            copy.wait()

    inner = (dot(low_ref[...], down_weight[...], NT) * slope_ref[...].astype(wide)).astype(low)
    inner_ref[...] = inner
    delta = delta_ref[...] + dot(inner, up_weight[...], NT)
    unit, scale = normalize(sum_ref[...])
    one = normalize_back(scale, unit, delta * vectors_ref[0:1, :])
    one_ref[...] = one
    one_low = one.astype(low)
    one_low_ref[...] = one_low
    mixed_ref[...] = dot(one_low, merge_weight[...], NT).astype(low)
    sums_ref[0:1, :] += jnp.sum(delta * unit, axis=0, keepdims=True)
    sums_ref[1:2, :] += jnp.sum(delta, axis=0, keepdims=True)


def inner_back(branch, delta, slope, total, vectors, merges, downs, ups, core, rows=256):
    count, hidden = slope.shape
    features = total.shape[1]
    block = pl.BlockSpec((rows, features), lambda i, c: (i, 0))
    tall = pl.BlockSpec((rows, hidden), lambda i, c: (i, 0))
    anywhere = pl.BlockSpec(memory_space=pl.ANY)
    return call(
        inner_kernel,
        "inner_back",
        (count // rows,),
        [
            block,
            block,
            tall,
            block,
            pl.BlockSpec(vectors.shape, lambda i, c: (0, 0)),
            *[anywhere] * 6,
        ],
        [tall, block, block, block, pl.BlockSpec((8, features), lambda i, c: (0, 0))],
        [
            shape((count, hidden)),
            shape((count, features), wide),
            shape((count, features)),
            shape((count, features)),
            shape((8, features), wide),
        ],
        [
            pltpu.VMEM((hidden, features), low),
            pltpu.VMEM((features, hidden), low),
            pltpu.VMEM((features, features), low),
            pltpu.SemaphoreType.DMA((3, 2)),
        ],
    )(core, branch, delta, slope, total, vectors, *merges, *downs, *ups)


def columns_kernel(core_ref, left_ref, own_ref, other_ref, keep_ref, give_ref):
    half = own_ref.shape[-1]
    both = jnp.concatenate([own_ref[...], other_ref[...]], axis=1)
    total = dot(left_ref[...], both, TN)
    keep_ref[...] = total[:, :half].astype(low)
    give_ref[...] = total[:, half:].astype(low)


def into_kernel(core_ref, left_ref, own_ref, other_ref, kept_ref, given_ref, keep_ref, give_ref):
    columns_kernel(core_ref, left_ref, own_ref, other_ref, keep_ref, give_ref)


def weight_into(left, right, keep, give, core):
    count, height = left.shape
    half = right.shape[1] // 2
    last = keep.shape[1] // half - 1
    out = pl.BlockSpec((height, half), lambda i, c: (0, last))
    return call(
        into_kernel,
        "weight_into",
        (1,),
        [
            pl.BlockSpec((count, height), lambda i, c: (0, 0)),
            pl.BlockSpec((count, half), lambda i, c: (0, c[0])),
            pl.BlockSpec((count, half), lambda i, c: (0, 1 - c[0])),
            pl.BlockSpec(memory_space=pl.ANY),
            pl.BlockSpec(memory_space=pl.ANY),
        ],
        [out, out],
        [shape(keep.shape)] * 2,
        aliases={4: 0, 5: 1},
    )(core, left, right, right, keep, give)


def weight_columns(left, right, core, rows=768):
    count, height = left.shape
    parts, _, width = right.shape
    half = width // 2
    steps = height // rows
    out = pl.BlockSpec((rows, half), lambda p, j, c: (j, p))
    return call(
        columns_kernel,
        "weight_columns",
        (parts, steps),
        [
            pl.BlockSpec((count, rows), lambda p, j, c: (0, j)),
            pl.BlockSpec((None, count, half), lambda p, j, c: (p, 0, c[0])),
            pl.BlockSpec((None, count, half), lambda p, j, c: (p, 0, 1 - c[0])),
        ],
        [out, out],
        [shape((height, parts * half))] * 2,
    )(core, left, right, right)


def wide_kernel(core_ref, left_ref, right_ref, keep_ref, give_ref):
    total = dot(left_ref[...], right_ref[...], TN).astype(low)

    @pl.when(pl.program_id(0) == 0)
    def _():
        give_ref[...] = total

    @pl.when(pl.program_id(0) == 1)
    def _():
        keep_ref[...] = total


def weight_wide(left, right, core, spare, columns=768):
    count, height = left.shape
    steps = right.shape[1] // 2 // columns
    return call(
        wide_kernel,
        "weight_wide",
        (2, steps),
        [
            pl.BlockSpec((count, height), lambda s, j, c: (0, 0)),
            pl.BlockSpec(
                (count, columns), lambda s, j, c: (0, j + steps * jnp.where(s == 0, 1 - c[0], c[0]))
            ),
        ],
        [
            pl.BlockSpec((height, columns), lambda s, j, c: (0, jnp.where(s == 1, j, 0))),
            pl.BlockSpec((height, columns), lambda s, j, c: (0, jnp.where(s == 0, j, steps - 1))),
        ],
        [shape((height, right.shape[1] // 2 + spare))] * 2,
    )(core, left, right)


def joined_kernel(core_ref, one_ref, left_ref, right_ref, own_ref, other_ref, out_ref, total):
    part = pl.program_id(1)

    @pl.when(part == 0)
    def _():
        total[...] = one_ref[...]

    both = jnp.concatenate([left_ref[...], right_ref[...]], axis=1)
    weight = jnp.concatenate([own_ref[...], other_ref[...]], axis=1)
    total[...] += dot(both, weight, NT)

    @pl.when(part == pl.num_programs(1) - 1)
    def _():
        out_ref[...] = total[...]


def joined_back(one, packed, own, other, core, rows=1024):
    count, features = one.shape
    parts = packed.shape[0]
    half = features // 2
    block = pl.BlockSpec((rows, features), lambda i, p, c: (i, 0))
    weight = pl.BlockSpec((features, half), lambda i, p, c: (0, p))
    return call(
        joined_kernel,
        "joined_back",
        (count // rows, parts),
        [
            block,
            pl.BlockSpec((None, rows, half), lambda i, p, c: (p, i, c[0])),
            pl.BlockSpec((None, rows, half), lambda i, p, c: (p, i, 1 - c[0])),
            weight,
            weight,
        ],
        block,
        shape((count, features), wide),
        [pltpu.VMEM((rows, features), wide)],
    )(core, one, packed, packed, own, other)


def pool_stats(left, right):
    total, size = left[0] + right[0], left[2] + right[2]
    center = total / size
    apart = (left[1] + right[1]) + (
        left[2] * jnp.square(left[0] / left[2] - center)
        + right[2] * jnp.square(right[0] / right[2] - center)
    )
    return jnp.stack([total, apart, size])


def shards(
    text_rows,
    visual_matrix,
    batch_gain,
    batch_shift,
    attend_weight,
    merge_weight,
    first_gain,
    first_shift,
    up_matrix,
    down_matrix,
    second_gain,
    second_shift,
    segment_counts,
    segment_ids,
    padding_mask,
    cotangent,
):
    docs, length, features = text_rows.shape
    count = docs * length
    hidden = up_matrix.shape[1]
    half = features // 2
    dp, fsdp = lax.axis_size("dp"), lax.axis_size("fsdp")
    core = lax.axis_index("dp") % 2
    which = core.reshape(1).astype(jnp.int32)
    piece = features // fsdp

    small = jnp.stack(
        [first_gain, first_shift, second_gain, second_shift, batch_gain, batch_shift]
    ).reshape(-1)
    first = jnp.concatenate(
        [
            half_of(visual_matrix, core),
            jnp.pad(small, (0, 16 * half - small.size)).reshape(16, half),
        ]
    )
    mine = jnp.concatenate(
        [
            half_of(attend_weight.reshape(piece, 3, features), core).reshape(piece, 3 * half),
            half_of(merge_weight, core),
        ],
        axis=1,
    )
    attend_own = gather_bulk(mine)
    attends = (attend_own, swap(attend_own, "dp", 1))
    first_own = spread(first, "fsdp", None, fsdp)
    first_other = swap(first_own, "dp", 1)
    direct = fsdp == 8
    up_half = half_of(up_matrix, core)
    if direct:
        chip = lax.axis_index("dp") // 2 % 2
        up_column = gather_line(after(half_of(up_half, chip), first_own))
    else:
        up_own = gather_bulk(up_half)
    down_own = gather_bulk(after(half_of(down_matrix, core), first_own))
    full_visual = join(first_own[:, :piece], first_other[:, :piece], core).reshape(features, features)
    small = first_own[:, piece:].reshape(fsdp, 16 * half)[:, : 6 * piece]
    small = small.reshape(fsdp, 6, piece).transpose(1, 0, 2).reshape(6, features)
    vectors = jnp.pad(small.astype(wide), ((0, 2), (0, 0)))
    full_batch_gain, full_batch_shift = vectors[4], vectors[5]

    slot_index = jnp.arange(SEGMAX)
    matches = segment_ids[:, :, None] == slot_index[None, None, :]
    onehot = matches.astype(low)
    onehot_wide = matches.astype(wide)
    divisor = jnp.maximum(jnp.sum(onehot_wide, axis=1), 1.0)[..., None]
    pooled_segments = (
        jnp.einsum("drs,drc->dsc", onehot, text_rows, preferred_element_type=wide) / divisor
    ).astype(low)
    visual_rows = jnp.einsum(
        "bil,ly->biy", pooled_segments, full_visual, preferred_element_type=wide
    )
    valid_slot = (slot_index[None, :] < segment_counts[:, None]).astype(wide)[..., None]
    local_count = jnp.sum(segment_counts).astype(wide)
    local_sum = jnp.sum(valid_slot * visual_rows, axis=(0, 1))
    local_center = visual_rows - local_sum / local_count
    local_square = jnp.sum(valid_slot * local_center * local_center, axis=(0, 1))
    stats = jnp.stack([local_sum, local_square, jnp.full_like(local_sum, local_count)])
    for axis in ("dp", "fsdp"):
        bit = 1
        while bit < lax.axis_size(axis):
            stats = pool_stats(stats, swap(stats, axis, bit))
            bit *= 2
    if direct:
        up_quarter = gather_side(after(up_column, stats))
    segment_total = stats[2]
    batch_center = stats[0] / segment_total
    center = visual_rows - batch_center
    variance = stats[1] / segment_total
    inverse_spread = lax.rsqrt(variance + eps_batch)
    normed = center * inverse_spread
    embedded = (normed * full_batch_gain + full_batch_shift).astype(low)
    joined = text_rows.astype(wide) + jnp.einsum(
        "drs,dsc->drc", onehot, embedded, preferred_element_type=wide
    )
    joined = joined.reshape(count, features)
    joined_low = joined.astype(low)
    if direct:
        joined_low, up_quarter = lax.optimization_barrier((joined_low, up_quarter))
        up_far = swap(up_quarter, "dp", 2)

    packed = project(joined_low, *attends, which).reshape(docs, length, -1)
    attended, share = attend(packed, padding_mask, which)
    flat_attended = attended.reshape(count, features)
    if direct:
        up_own = join(up_quarter, after(up_far, attended), chip)
    total_one, hidden_low = merge(flat_attended, joined, vectors, *attends, which)
    ups = (up_own, swap(up_own, "dp", 1))
    activated, slope = up(hidden_low, *ups, which)
    downs = (down_own, swap(after(down_own, activated), "dp", 1))
    layer_output, delta_two, branch_low, sums_two = down(
        activated, total_one, cotangent.reshape(count, features), vectors, *downs, which
    )

    down_halves = weight_columns(activated, branch_low[None], which)
    down_chip = add_low(down_halves[0], swap(down_halves[1], "dp", 1))
    down_chip, branch_low = lax.optimization_barrier((down_chip, branch_low))
    down_shard = finish(
        lax.psum_scatter(down_chip, "fsdp", scatter_dimension=0, tiled=True), core
    )
    delta_inner, delta_one, one_low, delta_attended, sums_one = inner_back(
        branch_low, delta_two, slope, total_one, vectors, attends, downs, ups, which
    )
    keep, give = weight_wide(hidden_low, delta_inner, which, half)
    keep, give = weight_into(flat_attended, one_low, keep, give, which)
    chip = add_low(keep, swap(give, "dp", 1))
    chip, delta_attended = lax.optimization_barrier((chip, delta_attended))
    up_merge_shard = finish(
        lax.psum_scatter(chip, "fsdp", scatter_dimension=0, tiled=True), core
    )
    delta_packed = attend_back(
        packed, share, delta_attended.reshape(docs, length, features), attended, which
    ).reshape(3, count, features)
    keep, give = weight_columns(joined_low, delta_packed, which)
    keep, give = scatter_begin(add_low(keep, swap(give, "dp", 1)))
    give, delta_packed = lax.optimization_barrier((give, delta_packed))
    given = swap(give, "fsdp", 1)
    delta_joined = joined_back(delta_one, delta_packed, *attends, which)
    attend_shard = scatter_end(keep, given, core)
    delta_joined = delta_joined.reshape(docs, length, features)
    delta_embedded = jnp.einsum(
        "drs,drc->dsc",
        onehot_wide,
        delta_joined,
        precision=highest_precision,
        preferred_element_type=wide,
    )
    sums = jnp.stack(
        [
            sums_one[0],
            sums_one[1],
            sums_two[0],
            sums_two[1],
            jnp.sum(delta_embedded * normed, axis=(0, 1)),
            jnp.sum(delta_embedded, axis=(0, 1)),
        ]
    )
    sums = sum_all(sums)
    gain_total, shift_total = sums[4], sums[5]
    visual_delta_rows = (
        valid_slot
        * full_batch_gain
        * inverse_spread
        * (delta_embedded - shift_total / segment_total - normed * gain_total / segment_total)
    ).astype(low)
    visual_local = jnp.einsum(
        "bli,blz->iz", pooled_segments, visual_delta_rows, preferred_element_type=wide
    ).astype(low)
    visual_shard = scatter_small(half_of(visual_local, core), half_of(visual_local, 1 - core), core)
    delta_pooled = (
        jnp.einsum("zbl,wl->zbw", visual_delta_rows, full_visual, preferred_element_type=wide)
        / divisor
    )
    text_gradient = delta_joined + jnp.einsum(
        "drs,dsc->drc",
        onehot_wide,
        delta_pooled,
        precision=highest_precision,
        preferred_element_type=wide,
    )

    own = lax.dynamic_slice_in_dim(sums, lax.axis_index("fsdp") * piece, piece, 1)
    attend_gradient = join(
        attend_shard[0].reshape(piece, 3, half), attend_shard[1].reshape(piece, 3, half), core
    ).reshape(piece, 3 * features)
    return (
        layer_output.reshape(docs, length, features),
        text_gradient,
        join(*visual_shard, core).astype(wide),
        own[4],
        own[5],
        attend_gradient.astype(wide),
        join(*(part[:, hidden // 2 :] for part in up_merge_shard), core).astype(wide),
        own[0],
        own[1],
        join(*(part[:, : hidden // 2] for part in up_merge_shard), core).astype(wide),
        join(*down_shard, core).astype(wide),
        own[2],
        own[3],
    )


def solution(mesh):
    in_specs = (
        P(("dp", "fsdp"), None, None),
        P("fsdp", None),
        P("fsdp"),
        P("fsdp"),
        P("fsdp", None),
        P("fsdp", None),
        P("fsdp"),
        P("fsdp"),
        P("fsdp", None),
        P("fsdp", None),
        P("fsdp"),
        P("fsdp"),
        P(("dp", "fsdp")),
        P(("dp", "fsdp"), None),
        P(("dp", "fsdp"), None),
        P(("dp", "fsdp"), None, None),
    )
    out_specs = (
        P(("dp", "fsdp"), None, None),
        P(("dp", "fsdp"), None, None),
        P("fsdp", None),
        P("fsdp"),
        P("fsdp"),
        P("fsdp", None),
        P("fsdp", None),
        P("fsdp"),
        P("fsdp"),
        P("fsdp", None),
        P("fsdp", None),
        P("fsdp"),
        P("fsdp"),
    )
    return jax.shard_map(shards, mesh=mesh, in_specs=in_specs, out_specs=out_specs, check_vma=False)
```

```python
import functools

import jax
import jax.numpy as jnp
from jax import lax
from jax.experimental import pallas as pl
from jax.experimental.pallas import tpu as pltpu
from jax.sharding import PartitionSpec as P

HEADS = 12
SEGMAX = 128
low = jnp.bfloat16
wide = jnp.float32
eps_norm = 1e-05
eps_batch = 1e-05
masked_score = -1e30
highest_precision = lax.Precision.HIGHEST

NN = (((1,), (0,)), ((), ()))
NT = (((1,), (1,)), ((), ()))
TN = (((0,), (0,)), ((), ()))

tail_spread = 0.39 * 2**-0.5
tail_poly = [
    0.5 * value
    for value in (
        0.22003657898400666,
        0.21993814342134163,
        0.20469834418114297,
        0.1590209501745049,
        0.17253866336379592,
        -0.06413901990527864,
        0.25209925299909935,
        -0.21837884731666118,
        0.05418596701413587,
    )
]


def dot(left, right, dims=NN):
    return lax.dot_general(left, right, dims, preferred_element_type=wide)


def shape(dims, dtype=low):
    return jax.ShapeDtypeStruct(dims, dtype)


def call(kernel, name, grid, in_specs, out_specs, out_shape, scratch=(), aliases=None):
    return pl.pallas_call(
        kernel,
        name=name,
        grid_spec=pltpu.PrefetchScalarGridSpec(
            num_scalar_prefetch=1,
            grid=grid,
            in_specs=in_specs,
            out_specs=out_specs,
            scratch_shapes=list(scratch),
        ),
        out_shape=out_shape,
        input_output_aliases=aliases or {},
        compiler_params=pltpu.CompilerParams(vmem_limit_bytes=56 * 2**20),
    )


def pair_groups(size):
    return [[i, i + 1] for i in range(0, size, 2)]


def line_groups(size):
    return [list(range(0, size, 2)), list(range(1, size, 2))]


def spread(value, axis, groups, count):
    copies = jnp.broadcast_to(value[None], (count,) + value.shape)
    return lax.all_to_all(copies, axis, 0, 0, axis_index_groups=groups)


def swap(value, axis, bit):
    size = lax.axis_size(axis)
    return lax.ppermute(value, axis, [(i, i ^ bit) for i in range(size)])


def half_of(value, index):
    half = value.shape[-1] // 2
    return lax.dynamic_slice_in_dim(value, index * half, half, value.ndim - 1)


def after(value, *others):
    return lax.optimization_barrier((value, *others))[0]


def gather_line(mine):
    line = lax.axis_index("fsdp") // 2
    around = [mine] + [
        lax.ppermute(mine, "fsdp", [(i, (i + 2 * step) % 8) for i in range(8)]) for step in (1, 2, 3)
    ]
    column = jnp.zeros((4,) + mine.shape, mine.dtype)
    for step in range(4):
        column = lax.dynamic_update_index_in_dim(column, around[step], (line - step) % 4, 0)
    return column


def gather_side(column):
    side = lax.axis_index("fsdp") % 2
    beside = swap(column, "fsdp", 1)
    own = jnp.where(
        side == 0, jnp.stack([column, beside], axis=1), jnp.stack([beside, column], axis=1)
    )
    return own.reshape(-1, column.shape[-1])


def gather_bulk(mine):
    return lax.all_gather(mine, "fsdp", axis=0, tiled=True)


def join(own, other, core):
    return jnp.where(
        core == 0,
        jnp.concatenate([own, other], axis=-1),
        jnp.concatenate([other, own], axis=-1),
    )


def add_low(left, right):
    return (left.astype(wide) + right.astype(wide)).astype(low)


def finish(total, core):
    bit = 2
    while bit < lax.axis_size("dp"):
        total = add_low(total, swap(total, "dp", bit))
        bit *= 2
    return total, swap(total, "dp", 1)


def scatter_small(keep, give, core):
    rows, half = keep.shape
    fsdp = lax.axis_size("fsdp")
    chip = add_low(keep, swap(give, "dp", 1)).reshape(fsdp, rows // fsdp, half)
    parts = lax.all_to_all(chip, "fsdp", 0, 0)
    return finish(jnp.sum(parts.astype(wide), axis=0).astype(low), core)


def scatter_begin(chip):
    rows, half = chip.shape
    fsdp = lax.axis_size("fsdp")
    side = lax.axis_index("fsdp") % 2
    chip = chip.reshape(fsdp // 2, 2, rows // fsdp, half)
    keep = lax.dynamic_index_in_dim(chip, side, 1, False)
    return keep, lax.dynamic_index_in_dim(chip, 1 - side, 1, False)


def scatter_end(keep, given, core):
    lines = keep.shape[0]
    line = lax.axis_index("fsdp") // 2
    pair = add_low(keep, given)
    total = lax.dynamic_index_in_dim(pair, line, 0, False).astype(wide)
    for step in range(1, lines):
        away = lax.dynamic_index_in_dim(pair, (line + step) % lines, 0, False)
        away = lax.ppermute(
            away, "fsdp", [(i, (i + 2 * step) % (2 * lines)) for i in range(2 * lines)]
        )
        total = total + away.astype(wide)
    return finish(total.astype(low), core)


def sum_all(value):
    for axis in ("dp", "fsdp"):
        bit = 1
        while bit < lax.axis_size(axis):
            value = value + swap(value, axis, bit)
            bit *= 2
    return value


def project_kernel(core_ref, x_ref, own_ref, other_ref, out_ref):
    half = own_ref.shape[1]
    both = jnp.concatenate([own_ref[...], other_ref[...]], axis=1)
    total = dot(x_ref[...], both).astype(low)
    out_ref[:, pl.ds(pl.multiple_of(core_ref[0] * half, 128), half)] = total[:, :half]
    out_ref[:, pl.ds(pl.multiple_of((1 - core_ref[0]) * half, 128), half)] = total[:, half:]


def project(x, own, other, core, rows=512):
    count, features = x.shape
    half = features // 2
    weight = pl.BlockSpec((features, half), lambda j, i, c: (0, j))
    return call(
        project_kernel,
        "project",
        (3, count // rows),
        [pl.BlockSpec((rows, features), lambda j, i, c: (i, 0)), weight, weight],
        pl.BlockSpec((rows, features), lambda j, i, c: (i, j)),
        shape((count, 3 * features)),
    )(core, x, own, other)


def attend_kernel(
    core_ref, q_ref, k_ref, v_ref, mask_ref, out_ref, share_ref, scores_ref, chunk=64
):
    queries, keys, values = q_ref[...], k_ref[...], v_ref[...]
    length = queries.shape[0]
    first = lax.broadcasted_iota(jnp.int32, queries.shape, 1) < queries.shape[1] // 2
    real = jnp.broadcast_to(mask_ref[...], (chunk, length)) > 0
    mixed = []
    for head in range(2):
        mine = first if head == 0 else jnp.logical_not(first)
        scaled = jnp.where(mine, queries, jnp.zeros_like(queries)) * jnp.asarray(0.125, low)
        scores_ref[head] = dot(scaled, keys, NT)
    for head in range(2):
        for row in range(0, length, chunk):
            scores = jnp.where(real, scores_ref[head, row : row + chunk], masked_score)
            raised = jnp.exp(scores - jnp.max(scores, axis=-1, keepdims=True))
            share = raised * (1.0 / jnp.sum(raised, axis=-1, keepdims=True))
            share_ref[head, row : row + chunk] = share.astype(low)
        mixed.append(dot(share_ref[head], values))
    out_ref[...] = jnp.where(first, mixed[0], mixed[1]).astype(low)


def column_spec(length, offset):
    return pl.BlockSpec((None, length, 128), lambda d, h, c: (d, 0, h + offset))


def attend(packed, mask, core):
    docs, length, columns = packed.shape
    pairs = columns // 3 // 128
    return call(
        attend_kernel,
        "attend",
        (docs, pairs),
        [
            column_spec(length, 0),
            column_spec(length, pairs),
            column_spec(length, 2 * pairs),
            pl.BlockSpec((None, 1, length), lambda d, h, c: (d, 0, 0)),
        ],
        [
            column_spec(length, 0),
            pl.BlockSpec((None, 2, length, length), lambda d, h, c: (d, h, 0, 0)),
        ],
        [
            shape((docs, length, columns // 3)),
            shape((docs, 2 * pairs, length, length)),
        ],
        [pltpu.VMEM((2, length, length), wide)],
    )(core, packed, packed, packed, mask[:, None, :])


def attend_back_kernel(core_ref, q_ref, k_ref, v_ref, share_ref, delta_ref, mixed_ref, out_ref):
    queries, keys, values, delta = q_ref[...], k_ref[...], v_ref[...], delta_ref[...]
    half = queries.shape[1] // 2
    first = lax.broadcasted_iota(jnp.int32, queries.shape, 1) < half
    product = delta.astype(wide) * mixed_ref[...].astype(wide)
    queries_t, delta_t = queries.T, delta.T
    for_queries, for_keys, for_values = [], [], []
    for head in range(2):
        mine = first if head == 0 else jnp.logical_not(first)
        delta_share = dot(jnp.where(mine, delta, jnp.zeros_like(delta)), values, NT)
        row = jnp.sum(jnp.where(mine, product, 0.0), axis=-1, keepdims=True)
        share = share_ref[head]
        delta_scores = (share.astype(wide) * (delta_share - row)).astype(low)
        for_queries.append(dot(delta_scores, keys))
        for_keys.append(dot(queries_t[half * head : half * (head + 1)], delta_scores))
        for_values.append(dot(delta_t[half * head : half * (head + 1)], share))
    out_ref[0] = (jnp.where(first, for_queries[0], for_queries[1]) * 0.125).astype(low)
    out_ref[1] = (jnp.concatenate(for_keys, 0) * 0.125).astype(low).T
    out_ref[2] = jnp.concatenate(for_values, 0).astype(low).T


def attend_back(packed, share, delta, mixed, core):
    docs, length, columns = packed.shape
    pairs = columns // 3 // 128
    return call(
        attend_back_kernel,
        "attend_back",
        (docs, pairs),
        [
            column_spec(length, 0),
            column_spec(length, pairs),
            column_spec(length, 2 * pairs),
            pl.BlockSpec((None, 2, length, length), lambda d, h, c: (d, h, 0, 0)),
            column_spec(length, 0),
            column_spec(length, 0),
        ],
        pl.BlockSpec((3, None, length, 128), lambda d, h, c: (0, d, 0, h)),
        shape((3, docs, length, columns // 3)),
    )(core, packed, packed, packed, share, delta, mixed)


def gelu_parts(value):
    ratio = 1.0 / (1.0 + tail_spread * jnp.abs(value))
    poly = tail_poly[-1]
    for coefficient in tail_poly[-2::-1]:
        poly = poly * ratio + coefficient
    bell = jnp.exp(-0.5 * value * value)
    tail = poly * ratio * bell
    below = jnp.where(value < 0, tail, 1.0 - tail)
    return value * below, below + value * (bell * 0.3989422804014327)


def up_kernel(core_ref, x_ref, own_ref, other_ref, out_ref, slope_ref, inner, chunk=16):
    def block(weight):
        inner[...] = dot(x_ref[...], weight)
        for row in range(0, inner.shape[0], chunk):
            value, slope = gelu_parts(inner[row : row + chunk])
            out_ref[row : row + chunk] = value.astype(low)
            slope_ref[row : row + chunk] = slope.astype(low)

    @pl.when(pl.program_id(0) == 0)
    def _():
        block(own_ref[...])

    @pl.when(pl.program_id(0) == 1)
    def _():
        block(other_ref[...])


def up(x, own, other, core, columns=768, rows=512):
    count, features = x.shape
    half = own.shape[1]
    steps = half // columns
    out = pl.BlockSpec(
        (rows, columns), lambda s, j, i, c: (i, j + steps * jnp.where(s == 0, c[0], 1 - c[0]))
    )
    return call(
        up_kernel,
        "up",
        (2, steps, count // rows),
        [
            pl.BlockSpec((rows, features), lambda s, j, i, c: (i, 0)),
            pl.BlockSpec((features, columns), lambda s, j, i, c: (0, jnp.where(s == 0, j, steps - 1))),
            pl.BlockSpec((features, columns), lambda s, j, i, c: (0, jnp.where(s == 1, j, 0))),
        ],
        [out, out],
        [shape((count, 2 * half))] * 2,
        [pltpu.VMEM((rows, columns), wide)],
    )(core, x, own, other)


def normalize(value):
    center = value - jnp.mean(value, axis=-1, keepdims=True)
    scale = lax.rsqrt(jnp.mean(center * center, axis=-1, keepdims=True) + eps_norm)
    return center * scale, scale


def normalize_back(scale, unit, delta):
    return scale * (
        delta
        - jnp.mean(delta, axis=-1, keepdims=True)
        - unit * jnp.mean(delta * unit, axis=-1, keepdims=True)
    )


def fetch(own, other, target, sems, core, start=0):
    half = target.shape[1] // 2
    own, other = own.at[:, pl.ds(start, half)], other.at[:, pl.ds(start, half)]
    mine = pl.multiple_of(core * half, 128)
    theirs = pl.multiple_of((1 - core) * half, 128)
    return (
        pltpu.make_async_copy(own, target.at[:, pl.ds(mine, half)], sems.at[0]),
        pltpu.make_async_copy(other, target.at[:, pl.ds(theirs, half)], sems.at[1]),
    )


def merge_kernel(
    core_ref, x_ref, joined_ref, vectors_ref, own_ref, other_ref, sum_ref, low_ref, weight, sems
):
    @pl.when(pl.program_id(0) == 0)
    def _():
        half = weight.shape[1] // 2
        copies = fetch(own_ref, other_ref, weight, sems, core_ref[0], 3 * half)
        for copy in copies:
            copy.start()
        for copy in copies:
            copy.wait()

    total = joined_ref[...] + dot(x_ref[...], weight[...])
    sum_ref[...] = total
    unit, _ = normalize(total)
    low_ref[...] = (unit * vectors_ref[0:1, :] + vectors_ref[1:2, :]).astype(low)


def merge(x, joined, vectors, own, other, core, rows=256):
    count, features = x.shape
    block = pl.BlockSpec((rows, features), lambda i, c: (i, 0))
    return call(
        merge_kernel,
        "merge",
        (count // rows,),
        [
            block,
            block,
            pl.BlockSpec(vectors.shape, lambda i, c: (0, 0)),
            pl.BlockSpec(memory_space=pl.ANY),
            pl.BlockSpec(memory_space=pl.ANY),
        ],
        [block, block],
        [shape((count, features), wide), shape((count, features))],
        [pltpu.VMEM((features, features), low), pltpu.SemaphoreType.DMA((2,))],
    )(core, x, joined, vectors, own, other)


def down_kernel(
    core_ref,
    x_ref,
    sum_ref,
    cotangent_ref,
    vectors_ref,
    own_ref,
    other_ref,
    out_ref,
    delta_ref,
    low_ref,
    sums_ref,
    weight,
    sems,
):
    @pl.when(pl.program_id(0) == 0)
    def _():
        copies = fetch(own_ref, other_ref, weight, sems, core_ref[0])
        for copy in copies:
            copy.start()
        sums_ref[...] = jnp.zeros_like(sums_ref)
        for copy in copies:
            copy.wait()

    unit, _ = normalize(sum_ref[...])
    hidden = unit * vectors_ref[0:1, :] + vectors_ref[1:2, :]
    unit, scale = normalize(hidden + dot(x_ref[...], weight[...]))
    out_ref[...] = unit * vectors_ref[2:3, :] + vectors_ref[3:4, :]
    given = cotangent_ref[...].astype(wide)
    delta = normalize_back(scale, unit, given * vectors_ref[2:3, :])
    delta_ref[...] = delta
    low_ref[...] = delta.astype(low)
    sums_ref[0:1, :] += jnp.sum(given * unit, axis=0, keepdims=True)
    sums_ref[1:2, :] += jnp.sum(given, axis=0, keepdims=True)


def down(x, total, cotangent, vectors, own, other, core, rows=256):
    count, hidden = x.shape
    features = total.shape[1]
    block = pl.BlockSpec((rows, features), lambda i, c: (i, 0))
    return call(
        down_kernel,
        "down",
        (count // rows,),
        [
            pl.BlockSpec((rows, hidden), lambda i, c: (i, 0)),
            block,
            block,
            pl.BlockSpec(vectors.shape, lambda i, c: (0, 0)),
            pl.BlockSpec(memory_space=pl.ANY),
            pl.BlockSpec(memory_space=pl.ANY),
        ],
        [block, block, block, pl.BlockSpec((8, features), lambda i, c: (0, 0))],
        [
            shape((count, features), wide),
            shape((count, features), wide),
            shape((count, features)),
            shape((8, features), wide),
        ],
        [pltpu.VMEM((hidden, features), low), pltpu.SemaphoreType.DMA((2,))],
    )(core, x, total, cotangent, vectors, own, other)


def inner_kernel(
    core_ref,
    low_ref,
    delta_ref,
    slope_ref,
    sum_ref,
    vectors_ref,
    merge_own_ref,
    merge_other_ref,
    down_own_ref,
    down_other_ref,
    up_own_ref,
    up_other_ref,
    inner_ref,
    one_ref,
    one_low_ref,
    mixed_ref,
    sums_ref,
    down_weight,
    up_weight,
    merge_weight,
    sems,
):
    core = core_ref[0]

    def copies():
        return (
            *fetch(down_own_ref, down_other_ref, down_weight, sems.at[0], core),
            *fetch(up_own_ref, up_other_ref, up_weight, sems.at[1], core),
            *fetch(
                merge_own_ref,
                merge_other_ref,
                merge_weight,
                sems.at[2],
                core,
                3 * merge_weight.shape[1] // 2,
            ),
        )

    @pl.when(pl.program_id(0) == 0)
    def _():
        started = copies()
        for copy in started:
            copy.start()
        sums_ref[...] = jnp.zeros_like(sums_ref)
        for copy in started:
            copy.wait()

    inner = (dot(low_ref[...], down_weight[...], NT) * slope_ref[...].astype(wide)).astype(low)
    inner_ref[...] = inner
    delta = delta_ref[...] + dot(inner, up_weight[...], NT)
    unit, scale = normalize(sum_ref[...])
    one = normalize_back(scale, unit, delta * vectors_ref[0:1, :])
    one_ref[...] = one
    one_low = one.astype(low)
    one_low_ref[...] = one_low
    mixed_ref[...] = dot(one_low, merge_weight[...], NT).astype(low)
    sums_ref[0:1, :] += jnp.sum(delta * unit, axis=0, keepdims=True)
    sums_ref[1:2, :] += jnp.sum(delta, axis=0, keepdims=True)


def inner_back(branch, delta, slope, total, vectors, merges, downs, ups, core, rows=256):
    count, hidden = slope.shape
    features = total.shape[1]
    block = pl.BlockSpec((rows, features), lambda i, c: (i, 0))
    tall = pl.BlockSpec((rows, hidden), lambda i, c: (i, 0))
    anywhere = pl.BlockSpec(memory_space=pl.ANY)
    return call(
        inner_kernel,
        "inner_back",
        (count // rows,),
        [
            block,
            block,
            tall,
            block,
            pl.BlockSpec(vectors.shape, lambda i, c: (0, 0)),
            *[anywhere] * 6,
        ],
        [tall, block, block, block, pl.BlockSpec((8, features), lambda i, c: (0, 0))],
        [
            shape((count, hidden)),
            shape((count, features), wide),
            shape((count, features)),
            shape((count, features)),
            shape((8, features), wide),
        ],
        [
            pltpu.VMEM((hidden, features), low),
            pltpu.VMEM((features, hidden), low),
            pltpu.VMEM((features, features), low),
            pltpu.SemaphoreType.DMA((3, 2)),
        ],
    )(core, branch, delta, slope, total, vectors, *merges, *downs, *ups)


def columns_kernel(core_ref, left_ref, own_ref, other_ref, keep_ref, give_ref):
    half = own_ref.shape[-1]
    both = jnp.concatenate([own_ref[...], other_ref[...]], axis=1)
    total = dot(left_ref[...], both, TN)
    keep_ref[...] = total[:, :half].astype(low)
    give_ref[...] = total[:, half:].astype(low)


def into_kernel(core_ref, left_ref, own_ref, other_ref, kept_ref, given_ref, keep_ref, give_ref):
    columns_kernel(core_ref, left_ref, own_ref, other_ref, keep_ref, give_ref)


def weight_into(left, right, keep, give, core):
    count, height = left.shape
    half = right.shape[1] // 2
    last = keep.shape[1] // half - 1
    out = pl.BlockSpec((height, half), lambda i, c: (0, last))
    return call(
        into_kernel,
        "weight_into",
        (1,),
        [
            pl.BlockSpec((count, height), lambda i, c: (0, 0)),
            pl.BlockSpec((count, half), lambda i, c: (0, c[0])),
            pl.BlockSpec((count, half), lambda i, c: (0, 1 - c[0])),
            pl.BlockSpec(memory_space=pl.ANY),
            pl.BlockSpec(memory_space=pl.ANY),
        ],
        [out, out],
        [shape(keep.shape)] * 2,
        aliases={4: 0, 5: 1},
    )(core, left, right, right, keep, give)


def weight_columns(left, right, core, rows=768):
    count, height = left.shape
    parts, _, width = right.shape
    half = width // 2
    steps = height // rows
    out = pl.BlockSpec((rows, half), lambda p, j, c: (j, p))
    return call(
        columns_kernel,
        "weight_columns",
        (parts, steps),
        [
            pl.BlockSpec((count, rows), lambda p, j, c: (0, j)),
            pl.BlockSpec((None, count, half), lambda p, j, c: (p, 0, c[0])),
            pl.BlockSpec((None, count, half), lambda p, j, c: (p, 0, 1 - c[0])),
        ],
        [out, out],
        [shape((height, parts * half))] * 2,
    )(core, left, right, right)


def wide_kernel(core_ref, left_ref, right_ref, keep_ref, give_ref):
    total = dot(left_ref[...], right_ref[...], TN).astype(low)

    @pl.when(pl.program_id(0) == 0)
    def _():
        give_ref[...] = total

    @pl.when(pl.program_id(0) == 1)
    def _():
        keep_ref[...] = total


def weight_wide(left, right, core, spare, columns=768):
    count, height = left.shape
    steps = right.shape[1] // 2 // columns
    return call(
        wide_kernel,
        "weight_wide",
        (2, steps),
        [
            pl.BlockSpec((count, height), lambda s, j, c: (0, 0)),
            pl.BlockSpec(
                (count, columns), lambda s, j, c: (0, j + steps * jnp.where(s == 0, 1 - c[0], c[0]))
            ),
        ],
        [
            pl.BlockSpec((height, columns), lambda s, j, c: (0, jnp.where(s == 1, j, 0))),
            pl.BlockSpec((height, columns), lambda s, j, c: (0, jnp.where(s == 0, j, steps - 1))),
        ],
        [shape((height, right.shape[1] // 2 + spare))] * 2,
    )(core, left, right)


def joined_kernel(core_ref, one_ref, left_ref, right_ref, own_ref, other_ref, out_ref, total):
    part = pl.program_id(1)

    @pl.when(part == 0)
    def _():
        total[...] = one_ref[...]

    both = jnp.concatenate([left_ref[...], right_ref[...]], axis=1)
    weight = jnp.concatenate([own_ref[...], other_ref[...]], axis=1)
    total[...] += dot(both, weight, NT)

    @pl.when(part == pl.num_programs(1) - 1)
    def _():
        out_ref[...] = total[...]


def joined_back(one, packed, own, other, core, rows=1024):
    count, features = one.shape
    parts = packed.shape[0]
    half = features // 2
    block = pl.BlockSpec((rows, features), lambda i, p, c: (i, 0))
    weight = pl.BlockSpec((features, half), lambda i, p, c: (0, p))
    return call(
        joined_kernel,
        "joined_back",
        (count // rows, parts),
        [
            block,
            pl.BlockSpec((None, rows, half), lambda i, p, c: (p, i, c[0])),
            pl.BlockSpec((None, rows, half), lambda i, p, c: (p, i, 1 - c[0])),
            weight,
            weight,
        ],
        block,
        shape((count, features), wide),
        [pltpu.VMEM((rows, features), wide)],
    )(core, one, packed, packed, own, other)


def pool_stats(left, right):
    total, size = left[0] + right[0], left[2] + right[2]
    center = total / size
    apart = (left[1] + right[1]) + (
        left[2] * jnp.square(left[0] / left[2] - center)
        + right[2] * jnp.square(right[0] / right[2] - center)
    )
    return jnp.stack([total, apart, size])


def shards(
    text_rows,
    visual_matrix,
    batch_gain,
    batch_shift,
    attend_weight,
    merge_weight,
    first_gain,
    first_shift,
    up_matrix,
    down_matrix,
    second_gain,
    second_shift,
    segment_counts,
    segment_ids,
    padding_mask,
    cotangent,
):
    docs, length, features = text_rows.shape
    count = docs * length
    hidden = up_matrix.shape[1]
    half = features // 2
    dp, fsdp = lax.axis_size("dp"), lax.axis_size("fsdp")
    core = lax.axis_index("dp") % 2
    which = core.reshape(1).astype(jnp.int32)
    piece = features // fsdp

    small = jnp.stack(
        [first_gain, first_shift, second_gain, second_shift, batch_gain, batch_shift]
    ).reshape(-1)
    first = jnp.concatenate(
        [
            half_of(visual_matrix, core),
            jnp.pad(small, (0, 16 * half - small.size)).reshape(16, half),
        ]
    )
    mine = jnp.concatenate(
        [
            half_of(attend_weight.reshape(piece, 3, features), core).reshape(piece, 3 * half),
            half_of(merge_weight, core),
        ],
        axis=1,
    )
    attend_own = gather_bulk(mine)
    attends = (attend_own, swap(attend_own, "dp", 1))
    first_own = spread(first, "fsdp", None, fsdp)
    first_other = swap(first_own, "dp", 1)
    direct = fsdp == 8
    up_half = half_of(up_matrix, core)
    if direct:
        chip = lax.axis_index("dp") // 2 % 2
        up_column = gather_line(after(half_of(up_half, chip), first_own))
    else:
        up_own = gather_bulk(up_half)
    down_own = gather_bulk(after(half_of(down_matrix, core), first_own))
    full_visual = join(first_own[:, :piece], first_other[:, :piece], core).reshape(features, features)
    small = first_own[:, piece:].reshape(fsdp, 16 * half)[:, : 6 * piece]
    small = small.reshape(fsdp, 6, piece).transpose(1, 0, 2).reshape(6, features)
    vectors = jnp.pad(small.astype(wide), ((0, 2), (0, 0)))
    full_batch_gain, full_batch_shift = vectors[4], vectors[5]

    slot_index = jnp.arange(SEGMAX)
    matches = segment_ids[:, :, None] == slot_index[None, None, :]
    onehot = matches.astype(low)
    onehot_wide = matches.astype(wide)
    divisor = jnp.maximum(jnp.sum(onehot_wide, axis=1), 1.0)[..., None]
    pooled_segments = (
        jnp.einsum("drs,drc->dsc", onehot, text_rows, preferred_element_type=wide) / divisor
    ).astype(low)
    visual_rows = jnp.einsum(
        "bil,ly->biy", pooled_segments, full_visual, preferred_element_type=wide
    )
    valid_slot = (slot_index[None, :] < segment_counts[:, None]).astype(wide)[..., None]
    local_count = jnp.sum(segment_counts).astype(wide)
    local_sum = jnp.sum(valid_slot * visual_rows, axis=(0, 1))
    local_center = visual_rows - local_sum / local_count
    local_square = jnp.sum(valid_slot * local_center * local_center, axis=(0, 1))
    stats = jnp.stack([local_sum, local_square, jnp.full_like(local_sum, local_count)])
    for axis in ("dp", "fsdp"):
        bit = 1
        while bit < lax.axis_size(axis):
            stats = pool_stats(stats, swap(stats, axis, bit))
            bit *= 2
    if direct:
        up_quarter = gather_side(after(up_column, stats))
    segment_total = stats[2]
    batch_center = stats[0] / segment_total
    center = visual_rows - batch_center
    variance = stats[1] / segment_total
    inverse_spread = lax.rsqrt(variance + eps_batch)
    normed = center * inverse_spread
    embedded = (normed * full_batch_gain + full_batch_shift).astype(low)
    joined = text_rows.astype(wide) + jnp.einsum(
        "drs,dsc->drc", onehot, embedded, preferred_element_type=wide
    )
    joined = joined.reshape(count, features)
    joined_low = joined.astype(low)
    if direct:
        joined_low, up_quarter = lax.optimization_barrier((joined_low, up_quarter))
        up_far = swap(up_quarter, "dp", 2)

    packed = project(joined_low, *attends, which).reshape(docs, length, -1)
    attended, share = attend(packed, padding_mask, which)
    flat_attended = attended.reshape(count, features)
    if direct:
        up_own = join(up_quarter, after(up_far, attended), chip)
    total_one, hidden_low = merge(flat_attended, joined, vectors, *attends, which)
    ups = (up_own, swap(up_own, "dp", 1))
    activated, slope = up(hidden_low, *ups, which)
    downs = (down_own, swap(after(down_own, activated), "dp", 1))
    layer_output, delta_two, branch_low, sums_two = down(
        activated, total_one, cotangent.reshape(count, features), vectors, *downs, which
    )

    down_halves = weight_columns(activated, branch_low[None], which)
    down_chip = add_low(down_halves[0], swap(down_halves[1], "dp", 1))
    down_chip, branch_low = lax.optimization_barrier((down_chip, branch_low))
    down_shard = finish(
        lax.psum_scatter(down_chip, "fsdp", scatter_dimension=0, tiled=True), core
    )
    delta_inner, delta_one, one_low, delta_attended, sums_one = inner_back(
        branch_low, delta_two, slope, total_one, vectors, attends, downs, ups, which
    )
    keep, give = weight_wide(hidden_low, delta_inner, which, half)
    keep, give = weight_into(flat_attended, one_low, keep, give, which)
    chip = add_low(keep, swap(give, "dp", 1))
    chip, delta_attended = lax.optimization_barrier((chip, delta_attended))
    up_merge_shard = finish(
        lax.psum_scatter(chip, "fsdp", scatter_dimension=0, tiled=True), core
    )
    delta_packed = attend_back(
        packed, share, delta_attended.reshape(docs, length, features), attended, which
    ).reshape(3, count, features)
    keep, give = weight_columns(joined_low, delta_packed, which)
    keep, give = scatter_begin(add_low(keep, swap(give, "dp", 1)))
    give, delta_packed = lax.optimization_barrier((give, delta_packed))
    given = swap(give, "fsdp", 1)
    delta_joined = joined_back(delta_one, delta_packed, *attends, which)
    attend_shard = scatter_end(keep, given, core)
    delta_joined = delta_joined.reshape(docs, length, features)
    delta_embedded = jnp.einsum(
        "drs,drc->dsc",
        onehot_wide,
        delta_joined,
        precision=highest_precision,
        preferred_element_type=wide,
    )
    sums = jnp.stack(
        [
            sums_one[0],
            sums_one[1],
            sums_two[0],
            sums_two[1],
            jnp.sum(delta_embedded * normed, axis=(0, 1)),
            jnp.sum(delta_embedded, axis=(0, 1)),
        ]
    )
    sums = sum_all(sums)
    gain_total, shift_total = sums[4], sums[5]
    visual_delta_rows = (
        valid_slot
        * full_batch_gain
        * inverse_spread
        * (delta_embedded - shift_total / segment_total - normed * gain_total / segment_total)
    ).astype(low)
    visual_local = jnp.einsum(
        "bli,blz->iz", pooled_segments, visual_delta_rows, preferred_element_type=wide
    ).astype(low)
    visual_shard = scatter_small(half_of(visual_local, core), half_of(visual_local, 1 - core), core)
    delta_pooled = (
        jnp.einsum("zbl,wl->zbw", visual_delta_rows, full_visual, preferred_element_type=wide)
        / divisor
    )
    text_gradient = delta_joined + jnp.einsum(
        "drs,dsc->drc",
        onehot_wide,
        delta_pooled,
        precision=highest_precision,
        preferred_element_type=wide,
    )

    own = lax.dynamic_slice_in_dim(sums, lax.axis_index("fsdp") * piece, piece, 1)
    attend_gradient = join(
        attend_shard[0].reshape(piece, 3, half), attend_shard[1].reshape(piece, 3, half), core
    ).reshape(piece, 3 * features)
    return (
        layer_output.reshape(docs, length, features),
        text_gradient,
        join(*visual_shard, core).astype(wide),
        own[4],
        own[5],
        attend_gradient.astype(wide),
        join(*(part[:, hidden // 2 :] for part in up_merge_shard), core).astype(wide),
        own[0],
        own[1],
        join(*(part[:, : hidden // 2] for part in up_merge_shard), core).astype(wide),
        join(*down_shard, core).astype(wide),
        own[2],
        own[3],
    )


def solution(mesh):
    in_specs = (
        P(("dp", "fsdp"), None, None),
        P("fsdp", None),
        P("fsdp"),
        P("fsdp"),
        P("fsdp", None),
        P("fsdp", None),
        P("fsdp"),
        P("fsdp"),
        P("fsdp", None),
        P("fsdp", None),
        P("fsdp"),
        P("fsdp"),
        P(("dp", "fsdp")),
        P(("dp", "fsdp"), None),
        P(("dp", "fsdp"), None),
        P(("dp", "fsdp"), None, None),
    )
    out_specs = (
        P(("dp", "fsdp"), None, None),
        P(("dp", "fsdp"), None, None),
        P("fsdp", None),
        P("fsdp"),
        P("fsdp"),
        P("fsdp", None),
        P("fsdp", None),
        P("fsdp"),
        P("fsdp"),
        P("fsdp", None),
        P("fsdp", None),
        P("fsdp"),
        P("fsdp"),
    )
    return jax.shard_map(shards, mesh=mesh, in_specs=in_specs, out_specs=out_specs, check_vma=False)
```

```python
import functools

import jax
import jax.numpy as jnp
from jax import lax
from jax.experimental import pallas as pl
from jax.experimental.pallas import tpu as pltpu
from jax.sharding import PartitionSpec as P

HEADS = 12
SEGMAX = 128
low = jnp.bfloat16
wide = jnp.float32
eps_norm = 1e-05
eps_batch = 1e-05
masked_score = -1e30
highest_precision = lax.Precision.HIGHEST

NN = (((1,), (0,)), ((), ()))
NT = (((1,), (1,)), ((), ()))
TN = (((0,), (0,)), ((), ()))

tail_spread = 0.39 * 2**-0.5
tail_poly = [
    0.5 * value
    for value in (
        0.22003657898400666,
        0.21993814342134163,
        0.20469834418114297,
        0.1590209501745049,
        0.17253866336379592,
        -0.06413901990527864,
        0.25209925299909935,
        -0.21837884731666118,
        0.05418596701413587,
    )
]


def dot(left, right, dims=NN):
    return lax.dot_general(left, right, dims, preferred_element_type=wide)


def shape(dims, dtype=low):
    return jax.ShapeDtypeStruct(dims, dtype)


def call(kernel, name, grid, in_specs, out_specs, out_shape, scratch=(), aliases=None):
    return pl.pallas_call(
        kernel,
        name=name,
        grid_spec=pltpu.PrefetchScalarGridSpec(
            num_scalar_prefetch=1,
            grid=grid,
            in_specs=in_specs,
            out_specs=out_specs,
            scratch_shapes=list(scratch),
        ),
        out_shape=out_shape,
        input_output_aliases=aliases or {},
        compiler_params=pltpu.CompilerParams(vmem_limit_bytes=56 * 2**20),
    )


def pair_groups(size):
    return [[i, i + 1] for i in range(0, size, 2)]


def line_groups(size):
    return [list(range(0, size, 2)), list(range(1, size, 2))]


def spread(value, axis, groups, count):
    copies = jnp.broadcast_to(value[None], (count,) + value.shape)
    return lax.all_to_all(copies, axis, 0, 0, axis_index_groups=groups)


def swap(value, axis, bit):
    size = lax.axis_size(axis)
    return lax.ppermute(value, axis, [(i, i ^ bit) for i in range(size)])


def half_of(value, index):
    half = value.shape[-1] // 2
    return lax.dynamic_slice_in_dim(value, index * half, half, value.ndim - 1)


def after(value, *others):
    return lax.optimization_barrier((value, *others))[0]


def gather_line(mine):
    line = lax.axis_index("fsdp") // 2
    around = [mine] + [
        lax.ppermute(mine, "fsdp", [(i, (i + 2 * step) % 8) for i in range(8)]) for step in (1, 2, 3)
    ]
    return jnp.stack([lax.select_n((line - row) % 4, *around) for row in range(4)])


def gather_side(column):
    side = lax.axis_index("fsdp") % 2
    beside = swap(column, "fsdp", 1)
    own = jnp.where(
        side == 0, jnp.stack([column, beside], axis=1), jnp.stack([beside, column], axis=1)
    )
    return own.reshape(-1, column.shape[-1])


def gather_bulk(mine):
    return lax.all_gather(mine, "fsdp", axis=0, tiled=True)


def join(own, other, core):
    return jnp.where(
        core == 0,
        jnp.concatenate([own, other], axis=-1),
        jnp.concatenate([other, own], axis=-1),
    )


def add_low(left, right):
    return (left.astype(wide) + right.astype(wide)).astype(low)


def finish(total, core):
    bit = 2
    while bit < lax.axis_size("dp"):
        total = add_low(total, swap(total, "dp", bit))
        bit *= 2
    return total, swap(total, "dp", 1)


def scatter_small(chip, core):
    rows, half = chip.shape
    fsdp = lax.axis_size("fsdp")
    parts = lax.all_to_all(chip.reshape(fsdp, rows // fsdp, half), "fsdp", 0, 0)
    return finish(jnp.sum(parts.astype(wide), axis=0).astype(low), core)


def scatter_begin(chip):
    rows, half = chip.shape
    fsdp = lax.axis_size("fsdp")
    side = lax.axis_index("fsdp") % 2
    chip = chip.reshape(fsdp // 2, 2, rows // fsdp, half)
    keep = lax.dynamic_index_in_dim(chip, side, 1, False)
    return keep, lax.dynamic_index_in_dim(chip, 1 - side, 1, False)


def scatter_end(keep, given, core):
    lines = keep.shape[0]
    line = lax.axis_index("fsdp") // 2
    pair = add_low(keep, given)
    total = lax.dynamic_index_in_dim(pair, line, 0, False).astype(wide)
    for step in range(1, lines):
        away = lax.dynamic_index_in_dim(pair, (line + step) % lines, 0, False)
        away = lax.ppermute(
            away, "fsdp", [(i, (i + 2 * step) % (2 * lines)) for i in range(2 * lines)]
        )
        total = total + away.astype(wide)
    return finish(total.astype(low), core)


def sum_axis(value, axis):
    bit = 1
    while bit < lax.axis_size(axis):
        value = value + swap(value, axis, bit)
        bit *= 2
    return value


def project_kernel(core_ref, x_ref, own_ref, other_ref, out_ref):
    half = own_ref.shape[1]
    both = jnp.concatenate([own_ref[...], other_ref[...]], axis=1)
    total = dot(x_ref[...], both).astype(low)
    out_ref[:, pl.ds(pl.multiple_of(core_ref[0] * half, 128), half)] = total[:, :half]
    out_ref[:, pl.ds(pl.multiple_of((1 - core_ref[0]) * half, 128), half)] = total[:, half:]


def project(x, own, other, core, rows=512):
    count, features = x.shape
    half = features // 2
    weight = pl.BlockSpec((features, half), lambda j, i, c: (0, j))
    return call(
        project_kernel,
        "project",
        (3, count // rows),
        [pl.BlockSpec((rows, features), lambda j, i, c: (i, 0)), weight, weight],
        pl.BlockSpec((rows, features), lambda j, i, c: (i, j)),
        shape((count, 3 * features)),
    )(core, x, own, other)


def attend_kernel(
    core_ref, q_ref, k_ref, v_ref, mask_ref, out_ref, share_ref, scores_ref, chunk=64
):
    queries, keys, values = q_ref[...], k_ref[...], v_ref[...]
    length = queries.shape[0]
    first = lax.broadcasted_iota(jnp.int32, queries.shape, 1) < queries.shape[1] // 2
    real = jnp.broadcast_to(mask_ref[...], (chunk, length)) > 0
    mixed = []
    for head in range(2):
        mine = first if head == 0 else jnp.logical_not(first)
        scaled = jnp.where(mine, queries, jnp.zeros_like(queries)) * jnp.asarray(0.125, low)
        scores_ref[head] = dot(scaled, keys, NT)
    for head in range(2):
        for row in range(0, length, chunk):
            scores = jnp.where(real, scores_ref[head, row : row + chunk], masked_score)
            raised = jnp.exp(scores - jnp.max(scores, axis=-1, keepdims=True))
            share = raised * (1.0 / jnp.sum(raised, axis=-1, keepdims=True))
            share_ref[head, row : row + chunk] = share.astype(low)
        mixed.append(dot(share_ref[head], values))
    out_ref[...] = jnp.where(first, mixed[0], mixed[1]).astype(low)


def column_spec(length, offset):
    return pl.BlockSpec((None, length, 128), lambda d, h, c: (d, 0, h + offset))


def attend(packed, mask, core):
    docs, length, columns = packed.shape
    pairs = columns // 3 // 128
    return call(
        attend_kernel,
        "attend",
        (docs, pairs),
        [
            column_spec(length, 0),
            column_spec(length, pairs),
            column_spec(length, 2 * pairs),
            pl.BlockSpec((None, 1, length), lambda d, h, c: (d, 0, 0)),
        ],
        [
            column_spec(length, 0),
            pl.BlockSpec((None, 2, length, length), lambda d, h, c: (d, h, 0, 0)),
        ],
        [
            shape((docs, length, columns // 3)),
            shape((docs, 2 * pairs, length, length)),
        ],
        [pltpu.VMEM((2, length, length), wide)],
    )(core, packed, packed, packed, mask[:, None, :])


def attend_back_kernel(core_ref, q_ref, k_ref, v_ref, share_ref, delta_ref, mixed_ref, out_ref):
    queries, keys, values, delta = q_ref[...], k_ref[...], v_ref[...], delta_ref[...]
    half = queries.shape[1] // 2
    first = lax.broadcasted_iota(jnp.int32, queries.shape, 1) < half
    product = delta.astype(wide) * mixed_ref[...].astype(wide)
    queries_t, delta_t = queries.T, delta.T
    for_queries, for_keys, for_values = [], [], []
    for head in range(2):
        mine = first if head == 0 else jnp.logical_not(first)
        delta_share = dot(jnp.where(mine, delta, jnp.zeros_like(delta)), values, NT)
        row = jnp.sum(jnp.where(mine, product, 0.0), axis=-1, keepdims=True)
        share = share_ref[head]
        delta_scores = (share.astype(wide) * (delta_share - row)).astype(low)
        for_queries.append(dot(delta_scores, keys))
        for_keys.append(dot(queries_t[half * head : half * (head + 1)], delta_scores))
        for_values.append(dot(delta_t[half * head : half * (head + 1)], share))
    out_ref[0] = (jnp.where(first, for_queries[0], for_queries[1]) * 0.125).astype(low)
    out_ref[1] = (jnp.concatenate(for_keys, 0) * 0.125).astype(low).T
    out_ref[2] = jnp.concatenate(for_values, 0).astype(low).T


def attend_back(packed, share, delta, mixed, core):
    docs, length, columns = packed.shape
    pairs = columns // 3 // 128
    return call(
        attend_back_kernel,
        "attend_back",
        (docs, pairs),
        [
            column_spec(length, 0),
            column_spec(length, pairs),
            column_spec(length, 2 * pairs),
            pl.BlockSpec((None, 2, length, length), lambda d, h, c: (d, h, 0, 0)),
            column_spec(length, 0),
            column_spec(length, 0),
        ],
        pl.BlockSpec((3, None, length, 128), lambda d, h, c: (0, d, 0, h)),
        shape((3, docs, length, columns // 3)),
    )(core, packed, packed, packed, share, delta, mixed)


def gelu_parts(value):
    ratio = 1.0 / (1.0 + tail_spread * jnp.abs(value))
    poly = tail_poly[-1]
    for coefficient in tail_poly[-2::-1]:
        poly = poly * ratio + coefficient
    bell = jnp.exp(-0.5 * value * value)
    tail = poly * ratio * bell
    below = jnp.where(value < 0, tail, 1.0 - tail)
    return value * below, below + value * (bell * 0.3989422804014327)


def up_kernel(core_ref, x_ref, own_ref, other_ref, out_ref, slope_ref, inner, chunk=16):
    def block(weight):
        inner[...] = dot(x_ref[...], weight)
        for row in range(0, inner.shape[0], chunk):
            value, slope = gelu_parts(inner[row : row + chunk])
            out_ref[row : row + chunk] = value.astype(low)
            slope_ref[row : row + chunk] = slope.astype(low)

    @pl.when(pl.program_id(0) == 0)
    def _():
        block(own_ref[...])

    @pl.when(pl.program_id(0) == 1)
    def _():
        block(other_ref[...])


def up(x, own, other, core, columns=768, rows=512):
    count, features = x.shape
    half = own.shape[1]
    steps = half // columns
    out = pl.BlockSpec(
        (rows, columns), lambda s, j, i, c: (i, j + steps * jnp.where(s == 0, c[0], 1 - c[0]))
    )
    return call(
        up_kernel,
        "up",
        (2, steps, count // rows),
        [
            pl.BlockSpec((rows, features), lambda s, j, i, c: (i, 0)),
            pl.BlockSpec((features, columns), lambda s, j, i, c: (0, jnp.where(s == 0, j, steps - 1))),
            pl.BlockSpec((features, columns), lambda s, j, i, c: (0, jnp.where(s == 1, j, 0))),
        ],
        [out, out],
        [shape((count, 2 * half))] * 2,
        [pltpu.VMEM((rows, columns), wide)],
    )(core, x, own, other)


def normalize(value):
    center = value - jnp.mean(value, axis=-1, keepdims=True)
    scale = lax.rsqrt(jnp.mean(center * center, axis=-1, keepdims=True) + eps_norm)
    return center * scale, scale


def normalize_back(scale, unit, delta):
    return scale * (
        delta
        - jnp.mean(delta, axis=-1, keepdims=True)
        - unit * jnp.mean(delta * unit, axis=-1, keepdims=True)
    )


def fetch(own, other, target, sems, core, start=0):
    half = target.shape[1] // 2
    own, other = own.at[:, pl.ds(start, half)], other.at[:, pl.ds(start, half)]
    mine = pl.multiple_of(core * half, 128)
    theirs = pl.multiple_of((1 - core) * half, 128)
    return (
        pltpu.make_async_copy(own, target.at[:, pl.ds(mine, half)], sems.at[0]),
        pltpu.make_async_copy(other, target.at[:, pl.ds(theirs, half)], sems.at[1]),
    )


def merge_kernel(
    core_ref, x_ref, joined_ref, vectors_ref, own_ref, other_ref, sum_ref, low_ref, weight, sems
):
    @pl.when(pl.program_id(0) == 0)
    def _():
        half = weight.shape[1] // 2
        copies = fetch(own_ref, other_ref, weight, sems, core_ref[0], 3 * half)
        for copy in copies:
            copy.start()
        for copy in copies:
            copy.wait()

    total = joined_ref[...] + dot(x_ref[...], weight[...])
    sum_ref[...] = total
    unit, _ = normalize(total)
    low_ref[...] = (unit * vectors_ref[0:1, :] + vectors_ref[1:2, :]).astype(low)


def merge(x, joined, vectors, own, other, core, rows=256):
    count, features = x.shape
    block = pl.BlockSpec((rows, features), lambda i, c: (i, 0))
    return call(
        merge_kernel,
        "merge",
        (count // rows,),
        [
            block,
            block,
            pl.BlockSpec(vectors.shape, lambda i, c: (0, 0)),
            pl.BlockSpec(memory_space=pl.ANY),
            pl.BlockSpec(memory_space=pl.ANY),
        ],
        [block, block],
        [shape((count, features), wide), shape((count, features))],
        [pltpu.VMEM((features, features), low), pltpu.SemaphoreType.DMA((2,))],
    )(core, x, joined, vectors, own, other)


def down_kernel(
    core_ref,
    x_ref,
    sum_ref,
    cotangent_ref,
    vectors_ref,
    own_ref,
    other_ref,
    out_ref,
    delta_ref,
    low_ref,
    sums_ref,
    weight,
    sems,
):
    @pl.when(pl.program_id(0) == 0)
    def _():
        copies = fetch(own_ref, other_ref, weight, sems, core_ref[0])
        for copy in copies:
            copy.start()
        sums_ref[...] = jnp.zeros_like(sums_ref)
        for copy in copies:
            copy.wait()

    unit, _ = normalize(sum_ref[...])
    hidden = unit * vectors_ref[0:1, :] + vectors_ref[1:2, :]
    unit, scale = normalize(hidden + dot(x_ref[...], weight[...]))
    out_ref[...] = unit * vectors_ref[2:3, :] + vectors_ref[3:4, :]
    given = cotangent_ref[...].astype(wide)
    delta = normalize_back(scale, unit, given * vectors_ref[2:3, :])
    delta_ref[...] = delta
    low_ref[...] = delta.astype(low)
    sums_ref[0:1, :] += jnp.sum(given * unit, axis=0, keepdims=True)
    sums_ref[1:2, :] += jnp.sum(given, axis=0, keepdims=True)


def down(x, total, cotangent, vectors, own, other, core, rows=256):
    count, hidden = x.shape
    features = total.shape[1]
    block = pl.BlockSpec((rows, features), lambda i, c: (i, 0))
    return call(
        down_kernel,
        "down",
        (count // rows,),
        [
            pl.BlockSpec((rows, hidden), lambda i, c: (i, 0)),
            block,
            block,
            pl.BlockSpec(vectors.shape, lambda i, c: (0, 0)),
            pl.BlockSpec(memory_space=pl.ANY),
            pl.BlockSpec(memory_space=pl.ANY),
        ],
        [block, block, block, pl.BlockSpec((8, features), lambda i, c: (0, 0))],
        [
            shape((count, features), wide),
            shape((count, features), wide),
            shape((count, features)),
            shape((8, features), wide),
        ],
        [pltpu.VMEM((hidden, features), low), pltpu.SemaphoreType.DMA((2,))],
    )(core, x, total, cotangent, vectors, own, other)


def inner_kernel(
    core_ref,
    low_ref,
    delta_ref,
    slope_ref,
    sum_ref,
    vectors_ref,
    merge_own_ref,
    merge_other_ref,
    down_own_ref,
    down_other_ref,
    up_own_ref,
    up_other_ref,
    inner_ref,
    one_ref,
    one_low_ref,
    mixed_ref,
    sums_ref,
    down_weight,
    up_weight,
    merge_weight,
    sems,
):
    core = core_ref[0]

    def copies():
        return (
            *fetch(down_own_ref, down_other_ref, down_weight, sems.at[0], core),
            *fetch(up_own_ref, up_other_ref, up_weight, sems.at[1], core),
            *fetch(
                merge_own_ref,
                merge_other_ref,
                merge_weight,
                sems.at[2],
                core,
                3 * merge_weight.shape[1] // 2,
            ),
        )

    @pl.when(pl.program_id(0) == 0)
    def _():
        started = copies()
        for copy in started:
            copy.start()
        sums_ref[...] = jnp.zeros_like(sums_ref)
        for copy in started:
            copy.wait()

    inner = (dot(low_ref[...], down_weight[...], NT) * slope_ref[...].astype(wide)).astype(low)
    inner_ref[...] = inner
    delta = delta_ref[...] + dot(inner, up_weight[...], NT)
    unit, scale = normalize(sum_ref[...])
    one = normalize_back(scale, unit, delta * vectors_ref[0:1, :])
    one_ref[...] = one
    one_low = one.astype(low)
    one_low_ref[...] = one_low
    mixed_ref[...] = dot(one_low, merge_weight[...], NT).astype(low)
    sums_ref[0:1, :] += jnp.sum(delta * unit, axis=0, keepdims=True)
    sums_ref[1:2, :] += jnp.sum(delta, axis=0, keepdims=True)


def inner_back(branch, delta, slope, total, vectors, merges, downs, ups, core, rows=256):
    count, hidden = slope.shape
    features = total.shape[1]
    block = pl.BlockSpec((rows, features), lambda i, c: (i, 0))
    tall = pl.BlockSpec((rows, hidden), lambda i, c: (i, 0))
    anywhere = pl.BlockSpec(memory_space=pl.ANY)
    return call(
        inner_kernel,
        "inner_back",
        (count // rows,),
        [
            block,
            block,
            tall,
            block,
            pl.BlockSpec(vectors.shape, lambda i, c: (0, 0)),
            *[anywhere] * 6,
        ],
        [tall, block, block, block, pl.BlockSpec((8, features), lambda i, c: (0, 0))],
        [
            shape((count, hidden)),
            shape((count, features), wide),
            shape((count, features)),
            shape((count, features)),
            shape((8, features), wide),
        ],
        [
            pltpu.VMEM((hidden, features), low),
            pltpu.VMEM((features, hidden), low),
            pltpu.VMEM((features, features), low),
            pltpu.SemaphoreType.DMA((3, 2)),
        ],
    )(core, branch, delta, slope, total, vectors, *merges, *downs, *ups)


def columns_kernel(core_ref, left_ref, own_ref, other_ref, keep_ref, give_ref):
    half = own_ref.shape[-1]
    both = jnp.concatenate([own_ref[...], other_ref[...]], axis=1)
    total = dot(left_ref[...], both, TN)
    keep_ref[...] = total[:, :half].astype(low)
    give_ref[...] = total[:, half:].astype(low)


def into_kernel(core_ref, left_ref, own_ref, other_ref, kept_ref, given_ref, keep_ref, give_ref):
    columns_kernel(core_ref, left_ref, own_ref, other_ref, keep_ref, give_ref)


def weight_into(left, right, keep, give, core):
    count, height = left.shape
    half = right.shape[1] // 2
    last = keep.shape[1] // half - 1
    out = pl.BlockSpec((height, half), lambda i, c: (0, last))
    return call(
        into_kernel,
        "weight_into",
        (1,),
        [
            pl.BlockSpec((count, height), lambda i, c: (0, 0)),
            pl.BlockSpec((count, half), lambda i, c: (0, c[0])),
            pl.BlockSpec((count, half), lambda i, c: (0, 1 - c[0])),
            pl.BlockSpec(memory_space=pl.ANY),
            pl.BlockSpec(memory_space=pl.ANY),
        ],
        [out, out],
        [shape(keep.shape)] * 2,
        aliases={4: 0, 5: 1},
    )(core, left, right, right, keep, give)


def weight_columns(left, right, core, rows=768):
    count, height = left.shape
    parts, _, width = right.shape
    half = width // 2
    steps = height // rows
    out = pl.BlockSpec((rows, half), lambda p, j, c: (j, p))
    return call(
        columns_kernel,
        "weight_columns",
        (parts, steps),
        [
            pl.BlockSpec((count, rows), lambda p, j, c: (0, j)),
            pl.BlockSpec((None, count, half), lambda p, j, c: (p, 0, c[0])),
            pl.BlockSpec((None, count, half), lambda p, j, c: (p, 0, 1 - c[0])),
        ],
        [out, out],
        [shape((height, parts * half))] * 2,
    )(core, left, right, right)


def wide_kernel(core_ref, left_ref, right_ref, keep_ref, give_ref):
    total = dot(left_ref[...], right_ref[...], TN).astype(low)

    @pl.when(pl.program_id(0) == 0)
    def _():
        give_ref[...] = total

    @pl.when(pl.program_id(0) == 1)
    def _():
        keep_ref[...] = total


def weight_wide(left, right, core, spare, columns=768):
    count, height = left.shape
    steps = right.shape[1] // 2 // columns
    return call(
        wide_kernel,
        "weight_wide",
        (2, steps),
        [
            pl.BlockSpec((count, height), lambda s, j, c: (0, 0)),
            pl.BlockSpec(
                (count, columns), lambda s, j, c: (0, j + steps * jnp.where(s == 0, 1 - c[0], c[0]))
            ),
        ],
        [
            pl.BlockSpec((height, columns), lambda s, j, c: (0, jnp.where(s == 1, j, 0))),
            pl.BlockSpec((height, columns), lambda s, j, c: (0, jnp.where(s == 0, j, steps - 1))),
        ],
        [shape((height, right.shape[1] // 2 + spare))] * 2,
    )(core, left, right)


def joined_kernel(core_ref, one_ref, left_ref, right_ref, own_ref, other_ref, out_ref, total):
    part = pl.program_id(1)

    @pl.when(part == 0)
    def _():
        total[...] = one_ref[...]

    both = jnp.concatenate([left_ref[...], right_ref[...]], axis=1)
    weight = jnp.concatenate([own_ref[...], other_ref[...]], axis=1)
    total[...] += dot(both, weight, NT)

    @pl.when(part == pl.num_programs(1) - 1)
    def _():
        out_ref[...] = total[...]


def joined_back(one, packed, own, other, core, rows=1024):
    count, features = one.shape
    parts = packed.shape[0]
    half = features // 2
    block = pl.BlockSpec((rows, features), lambda i, p, c: (i, 0))
    weight = pl.BlockSpec((features, half), lambda i, p, c: (0, p))
    return call(
        joined_kernel,
        "joined_back",
        (count // rows, parts),
        [
            block,
            pl.BlockSpec((None, rows, half), lambda i, p, c: (p, i, c[0])),
            pl.BlockSpec((None, rows, half), lambda i, p, c: (p, i, 1 - c[0])),
            weight,
            weight,
        ],
        block,
        shape((count, features), wide),
        [pltpu.VMEM((rows, features), wide)],
    )(core, one, packed, packed, own, other)


def pool_stats(left, right):
    total, size = left[0] + right[0], left[2] + right[2]
    center = total / size
    apart = (left[1] + right[1]) + (
        left[2] * jnp.square(left[0] / left[2] - center)
        + right[2] * jnp.square(right[0] / right[2] - center)
    )
    return jnp.stack([total, apart, size])


def shards(
    text_rows,
    visual_matrix,
    batch_gain,
    batch_shift,
    attend_weight,
    merge_weight,
    first_gain,
    first_shift,
    up_matrix,
    down_matrix,
    second_gain,
    second_shift,
    segment_counts,
    segment_ids,
    padding_mask,
    cotangent,
):
    docs, length, features = text_rows.shape
    count = docs * length
    hidden = up_matrix.shape[1]
    half = features // 2
    dp, fsdp = lax.axis_size("dp"), lax.axis_size("fsdp")
    core = lax.axis_index("dp") % 2
    which = core.reshape(1).astype(jnp.int32)
    piece = features // fsdp

    small = jnp.stack(
        [first_gain, first_shift, second_gain, second_shift, batch_gain, batch_shift]
    ).reshape(-1)
    first = jnp.concatenate(
        [
            half_of(visual_matrix, core),
            jnp.pad(small, (0, 16 * half - small.size)).reshape(16, half),
        ]
    )
    mine = jnp.concatenate(
        [
            half_of(attend_weight.reshape(piece, 3, features), core).reshape(piece, 3 * half),
            half_of(merge_weight, core),
        ],
        axis=1,
    )
    attend_own = gather_bulk(mine)
    attends = (attend_own, swap(attend_own, "dp", 1))
    first_own = spread(first, "fsdp", None, fsdp)
    first_other = swap(first_own, "dp", 1)
    direct = fsdp == 8
    up_half = half_of(up_matrix, core)
    if direct:
        chip = lax.axis_index("dp") // 2 % 2
        up_column = gather_line(after(half_of(up_half, chip), first_own))
    else:
        up_own = gather_bulk(up_half)
    down_own = gather_bulk(after(half_of(down_matrix, core), first_own))
    full_visual = join(first_own[:, :piece], first_other[:, :piece], core).reshape(features, features)
    small = first_own[:, piece:].reshape(fsdp, 16 * half)[:, : 6 * piece]
    small = small.reshape(fsdp, 6, piece).transpose(1, 0, 2).reshape(6, features)
    vectors = jnp.pad(small.astype(wide), ((0, 2), (0, 0)))
    full_batch_gain, full_batch_shift = vectors[4], vectors[5]

    slot_index = jnp.arange(SEGMAX)
    matches = segment_ids[:, :, None] == slot_index[None, None, :]
    onehot = matches.astype(low)
    onehot_wide = matches.astype(wide)
    divisor = jnp.maximum(jnp.sum(onehot_wide, axis=1), 1.0)[..., None]
    pooled_segments = (
        jnp.einsum("drs,drc->dsc", onehot, text_rows, preferred_element_type=wide) / divisor
    ).astype(low)
    visual_rows = jnp.einsum(
        "bil,ly->biy", pooled_segments, full_visual, preferred_element_type=wide
    )
    valid_slot = (slot_index[None, :] < segment_counts[:, None]).astype(wide)[..., None]
    local_count = jnp.sum(segment_counts).astype(wide)
    local_sum = jnp.sum(valid_slot * visual_rows, axis=(0, 1))
    local_center = visual_rows - local_sum / local_count
    local_square = jnp.sum(valid_slot * local_center * local_center, axis=(0, 1))
    stats = jnp.stack([local_sum, local_square, jnp.full_like(local_sum, local_count)])
    for axis in ("dp", "fsdp"):
        bit = 1
        while bit < lax.axis_size(axis):
            stats = pool_stats(stats, swap(stats, axis, bit))
            bit *= 2
    if direct:
        up_quarter = gather_side(after(up_column, stats))
    segment_total = stats[2]
    batch_center = stats[0] / segment_total
    center = visual_rows - batch_center
    variance = stats[1] / segment_total
    inverse_spread = lax.rsqrt(variance + eps_batch)
    normed = center * inverse_spread
    embedded = (normed * full_batch_gain + full_batch_shift).astype(low)
    joined = text_rows.astype(wide) + jnp.einsum(
        "drs,dsc->drc", onehot, embedded, preferred_element_type=wide
    )
    joined = joined.reshape(count, features)
    joined_low = joined.astype(low)
    if direct:
        joined_low, up_quarter = lax.optimization_barrier((joined_low, up_quarter))
        up_far = swap(up_quarter, "dp", 2)

    packed = project(joined_low, *attends, which).reshape(docs, length, -1)
    attended, share = attend(packed, padding_mask, which)
    flat_attended = attended.reshape(count, features)
    if direct:
        up_own = join(up_quarter, after(up_far, attended), chip)
    total_one, hidden_low = merge(flat_attended, joined, vectors, *attends, which)
    ups = (up_own, swap(up_own, "dp", 1))
    activated, slope = up(hidden_low, *ups, which)
    downs = (down_own, swap(after(down_own, activated), "dp", 1))
    layer_output, delta_two, branch_low, sums_two = down(
        activated, total_one, cotangent.reshape(count, features), vectors, *downs, which
    )

    down_halves = weight_columns(activated, branch_low[None], which)
    down_chip = add_low(down_halves[0], swap(down_halves[1], "dp", 1))
    down_chip, branch_low = lax.optimization_barrier((down_chip, branch_low))
    down_sum = lax.psum_scatter(down_chip, "fsdp", scatter_dimension=0, tiled=True)
    delta_inner, delta_one, one_low, delta_attended, sums_one = inner_back(
        branch_low, delta_two, slope, total_one, vectors, attends, downs, ups, which
    )
    keep, give = weight_wide(hidden_low, delta_inner, which, half)
    keep, give = weight_into(flat_attended, one_low, keep, give, which)
    chip = add_low(keep, swap(give, "dp", 1))
    chip, delta_attended = lax.optimization_barrier((chip, delta_attended))
    up_merge_sum = lax.psum_scatter(chip, "fsdp", scatter_dimension=0, tiled=True)
    delta_packed = attend_back(
        packed, share, delta_attended.reshape(docs, length, features), attended, which
    ).reshape(3, count, features)
    down_sum, delta_packed = lax.optimization_barrier((down_sum, delta_packed))
    delta_joined = joined_back(delta_one, delta_packed, *attends, which)
    delta_joined = delta_joined.reshape(docs, length, features)
    delta_embedded = jnp.einsum(
        "drs,drc->dsc",
        onehot_wide,
        delta_joined,
        precision=highest_precision,
        preferred_element_type=wide,
    )
    sums = jnp.stack(
        [
            sums_one[0],
            sums_one[1],
            sums_two[0],
            sums_two[1],
            jnp.sum(delta_embedded * normed, axis=(0, 1)),
            jnp.sum(delta_embedded, axis=(0, 1)),
        ]
    )
    keep, give = weight_columns(joined_low, after(delta_packed, sums), which)
    sums, give = lax.optimization_barrier((sum_axis(sums, "dp"), give))
    sums = sum_axis(sums, "fsdp")
    up_merge_shard = finish(after(up_merge_sum, sums), core)
    down_shard = finish(after(down_sum, sums), core)
    attend_keep, attend_give = scatter_begin(add_low(keep, swap(give, "dp", 1)))
    attend_given = swap(attend_give, "fsdp", 1)
    gain_total, shift_total = sums[4], sums[5]
    visual_delta_rows = (
        valid_slot
        * full_batch_gain
        * inverse_spread
        * (delta_embedded - shift_total / segment_total - normed * gain_total / segment_total)
    ).astype(low)
    visual_local = jnp.einsum(
        "bli,blz->iz", pooled_segments, visual_delta_rows, preferred_element_type=wide
    ).astype(low)
    visual_chip = add_low(half_of(visual_local, core), swap(half_of(visual_local, 1 - core), "dp", 1))
    visual_shard = scatter_small(visual_chip, core)
    attend_shard = scatter_end(attend_keep, after(attend_given, visual_chip), core)
    delta_pooled = (
        jnp.einsum("zbl,wl->zbw", visual_delta_rows, full_visual, preferred_element_type=wide)
        / divisor
    )
    text_gradient = delta_joined + jnp.einsum(
        "drs,dsc->drc",
        onehot_wide,
        delta_pooled,
        precision=highest_precision,
        preferred_element_type=wide,
    )

    own = lax.dynamic_slice_in_dim(sums, lax.axis_index("fsdp") * piece, piece, 1)
    attend_gradient = join(
        attend_shard[0].reshape(piece, 3, half), attend_shard[1].reshape(piece, 3, half), core
    ).reshape(piece, 3 * features)
    return (
        layer_output.reshape(docs, length, features),
        text_gradient,
        join(*visual_shard, core).astype(wide),
        own[4],
        own[5],
        attend_gradient.astype(wide),
        join(*(part[:, hidden // 2 :] for part in up_merge_shard), core).astype(wide),
        own[0],
        own[1],
        join(*(part[:, : hidden // 2] for part in up_merge_shard), core).astype(wide),
        join(*down_shard, core).astype(wide),
        own[2],
        own[3],
    )


def solution(mesh):
    in_specs = (
        P(("dp", "fsdp"), None, None),
        P("fsdp", None),
        P("fsdp"),
        P("fsdp"),
        P("fsdp", None),
        P("fsdp", None),
        P("fsdp"),
        P("fsdp"),
        P("fsdp", None),
        P("fsdp", None),
        P("fsdp"),
        P("fsdp"),
        P(("dp", "fsdp")),
        P(("dp", "fsdp"), None),
        P(("dp", "fsdp"), None),
        P(("dp", "fsdp"), None, None),
    )
    out_specs = (
        P(("dp", "fsdp"), None, None),
        P(("dp", "fsdp"), None, None),
        P("fsdp", None),
        P("fsdp"),
        P("fsdp"),
        P("fsdp", None),
        P("fsdp", None),
        P("fsdp"),
        P("fsdp"),
        P("fsdp", None),
        P("fsdp", None),
        P("fsdp"),
        P("fsdp"),
    )
    return jax.shard_map(shards, mesh=mesh, in_specs=in_specs, out_specs=out_specs, check_vma=False)
```

```python
import functools

import jax
import jax.numpy as jnp
from jax import lax
from jax.experimental import pallas as pl
from jax.experimental.pallas import tpu as pltpu
from jax.sharding import PartitionSpec as P

HEADS = 12
SEGMAX = 128
low = jnp.bfloat16
wide = jnp.float32
eps_norm = 1e-05
eps_batch = 1e-05
masked_score = -1e30
highest_precision = lax.Precision.HIGHEST

NN = (((1,), (0,)), ((), ()))
NT = (((1,), (1,)), ((), ()))
TN = (((0,), (0,)), ((), ()))

tail_spread = 0.39 * 2**-0.5
tail_poly = [
    0.5 * value
    for value in (
        0.22003657898400666,
        0.21993814342134163,
        0.20469834418114297,
        0.1590209501745049,
        0.17253866336379592,
        -0.06413901990527864,
        0.25209925299909935,
        -0.21837884731666118,
        0.05418596701413587,
    )
]


def dot(left, right, dims=NN):
    return lax.dot_general(left, right, dims, preferred_element_type=wide)


def shape(dims, dtype=low):
    return jax.ShapeDtypeStruct(dims, dtype)


def call(kernel, name, grid, in_specs, out_specs, out_shape, scratch=(), aliases=None):
    return pl.pallas_call(
        kernel,
        name=name,
        grid_spec=pltpu.PrefetchScalarGridSpec(
            num_scalar_prefetch=1,
            grid=grid,
            in_specs=in_specs,
            out_specs=out_specs,
            scratch_shapes=list(scratch),
        ),
        out_shape=out_shape,
        input_output_aliases=aliases or {},
        compiler_params=pltpu.CompilerParams(vmem_limit_bytes=56 * 2**20),
    )


def pair_groups(size):
    return [[i, i + 1] for i in range(0, size, 2)]


def line_groups(size):
    return [list(range(0, size, 2)), list(range(1, size, 2))]


def spread(value, axis, groups, count):
    copies = jnp.broadcast_to(value[None], (count,) + value.shape)
    return lax.all_to_all(copies, axis, 0, 0, axis_index_groups=groups)


def swap(value, axis, bit):
    size = lax.axis_size(axis)
    return lax.ppermute(value, axis, [(i, i ^ bit) for i in range(size)])


def half_of(value, index):
    half = value.shape[-1] // 2
    return lax.dynamic_slice_in_dim(value, index * half, half, value.ndim - 1)


def after(value, *others):
    return lax.optimization_barrier((value, *others))[0]


def gather_line(mine):
    line = lax.axis_index("fsdp") // 2
    around = [mine] + [
        lax.ppermute(mine, "fsdp", [(i, (i + 2 * step) % 8) for i in range(8)]) for step in (1, 2, 3)
    ]
    column = jnp.zeros((4,) + mine.shape, mine.dtype)
    for step in range(4):
        column = lax.dynamic_update_index_in_dim(column, around[step], (line - step) % 4, 0)
    return column


def gather_side(column):
    side = lax.axis_index("fsdp") % 2
    beside = swap(column, "fsdp", 1)
    own = jnp.where(
        side == 0, jnp.stack([column, beside], axis=1), jnp.stack([beside, column], axis=1)
    )
    return own.reshape(-1, column.shape[-1])


def gather_bulk(mine):
    return lax.all_gather(mine, "fsdp", axis=0, tiled=True)


def join(own, other, core):
    return jnp.where(
        core == 0,
        jnp.concatenate([own, other], axis=-1),
        jnp.concatenate([other, own], axis=-1),
    )


def add_low(left, right):
    return (left.astype(wide) + right.astype(wide)).astype(low)


def finish(total, core):
    bit = 2
    while bit < lax.axis_size("dp"):
        total = add_low(total, swap(total, "dp", bit))
        bit *= 2
    return total, swap(total, "dp", 1)


def scatter_small(keep, give, core):
    rows, half = keep.shape
    fsdp = lax.axis_size("fsdp")
    chip = add_low(keep, swap(give, "dp", 1)).reshape(fsdp, rows // fsdp, half)
    parts = lax.all_to_all(chip, "fsdp", 0, 0)
    return finish(jnp.sum(parts.astype(wide), axis=0).astype(low), core)


def scatter_begin(chip):
    rows, half = chip.shape
    fsdp = lax.axis_size("fsdp")
    side = lax.axis_index("fsdp") % 2
    chip = chip.reshape(fsdp // 2, 2, rows // fsdp, half)
    keep = lax.dynamic_index_in_dim(chip, side, 1, False)
    return keep, lax.dynamic_index_in_dim(chip, 1 - side, 1, False)


def scatter_end(keep, given, core):
    lines = keep.shape[0]
    line = lax.axis_index("fsdp") // 2
    pair = add_low(keep, given)
    total = lax.dynamic_index_in_dim(pair, line, 0, False).astype(wide)
    for step in range(1, lines):
        away = lax.dynamic_index_in_dim(pair, (line + step) % lines, 0, False)
        away = lax.ppermute(
            away, "fsdp", [(i, (i + 2 * step) % (2 * lines)) for i in range(2 * lines)]
        )
        total = total + away.astype(wide)
    return finish(total.astype(low), core)


def sum_all(value):
    for axis in ("dp", "fsdp"):
        bit = 1
        while bit < lax.axis_size(axis):
            value = value + swap(value, axis, bit)
            bit *= 2
    return value


def project_kernel(core_ref, x_ref, own_ref, other_ref, out_ref):
    half = own_ref.shape[1]
    both = jnp.concatenate([own_ref[...], other_ref[...]], axis=1)
    total = dot(x_ref[...], both).astype(low)
    out_ref[:, pl.ds(pl.multiple_of(core_ref[0] * half, 128), half)] = total[:, :half]
    out_ref[:, pl.ds(pl.multiple_of((1 - core_ref[0]) * half, 128), half)] = total[:, half:]


def project(x, own, other, core, rows=512):
    count, features = x.shape
    half = features // 2
    weight = pl.BlockSpec((features, half), lambda j, i, c: (0, j))
    return call(
        project_kernel,
        "project",
        (3, count // rows),
        [pl.BlockSpec((rows, features), lambda j, i, c: (i, 0)), weight, weight],
        pl.BlockSpec((rows, features), lambda j, i, c: (i, j)),
        shape((count, 3 * features)),
    )(core, x, own, other)


def attend_kernel(
    core_ref, q_ref, k_ref, v_ref, mask_ref, out_ref, share_ref, scores_ref, chunk=64
):
    queries, keys, values = q_ref[...], k_ref[...], v_ref[...]
    length = queries.shape[0]
    first = lax.broadcasted_iota(jnp.int32, queries.shape, 1) < queries.shape[1] // 2
    real = jnp.broadcast_to(mask_ref[...], (chunk, length)) > 0
    mixed = []
    for head in range(2):
        mine = first if head == 0 else jnp.logical_not(first)
        scaled = jnp.where(mine, queries, jnp.zeros_like(queries)) * jnp.asarray(0.125, low)
        scores_ref[head] = dot(scaled, keys, NT)
    for head in range(2):
        for row in range(0, length, chunk):
            scores = jnp.where(real, scores_ref[head, row : row + chunk], masked_score)
            raised = jnp.exp(scores - jnp.max(scores, axis=-1, keepdims=True))
            share = raised * (1.0 / jnp.sum(raised, axis=-1, keepdims=True))
            share_ref[head, row : row + chunk] = share.astype(low)
        mixed.append(dot(share_ref[head], values))
    out_ref[...] = jnp.where(first, mixed[0], mixed[1]).astype(low)


def column_spec(length, offset):
    return pl.BlockSpec((None, length, 128), lambda d, h, c: (d, 0, h + offset))


def attend(packed, mask, core):
    docs, length, columns = packed.shape
    pairs = columns // 3 // 128
    return call(
        attend_kernel,
        "attend",
        (docs, pairs),
        [
            column_spec(length, 0),
            column_spec(length, pairs),
            column_spec(length, 2 * pairs),
            pl.BlockSpec((None, 1, length), lambda d, h, c: (d, 0, 0)),
        ],
        [
            column_spec(length, 0),
            pl.BlockSpec((None, 2, length, length), lambda d, h, c: (d, h, 0, 0)),
        ],
        [
            shape((docs, length, columns // 3)),
            shape((docs, 2 * pairs, length, length)),
        ],
        [pltpu.VMEM((2, length, length), wide)],
    )(core, packed, packed, packed, mask[:, None, :])


def attend_back_kernel(core_ref, q_ref, k_ref, v_ref, share_ref, delta_ref, mixed_ref, out_ref):
    queries, keys, values, delta = q_ref[...], k_ref[...], v_ref[...], delta_ref[...]
    half = queries.shape[1] // 2
    first = lax.broadcasted_iota(jnp.int32, queries.shape, 1) < half
    product = delta.astype(wide) * mixed_ref[...].astype(wide)
    queries_t, delta_t = queries.T, delta.T
    for_queries, for_keys, for_values = [], [], []
    for head in range(2):
        mine = first if head == 0 else jnp.logical_not(first)
        delta_share = dot(jnp.where(mine, delta, jnp.zeros_like(delta)), values, NT)
        row = jnp.sum(jnp.where(mine, product, 0.0), axis=-1, keepdims=True)
        share = share_ref[head]
        delta_scores = (share.astype(wide) * (delta_share - row)).astype(low)
        for_queries.append(dot(delta_scores, keys))
        for_keys.append(dot(queries_t[half * head : half * (head + 1)], delta_scores))
        for_values.append(dot(delta_t[half * head : half * (head + 1)], share))
    out_ref[0] = (jnp.where(first, for_queries[0], for_queries[1]) * 0.125).astype(low)
    out_ref[1] = (jnp.concatenate(for_keys, 0) * 0.125).astype(low).T
    out_ref[2] = jnp.concatenate(for_values, 0).astype(low).T


def attend_back(packed, share, delta, mixed, core):
    docs, length, columns = packed.shape
    pairs = columns // 3 // 128
    return call(
        attend_back_kernel,
        "attend_back",
        (docs, pairs),
        [
            column_spec(length, 0),
            column_spec(length, pairs),
            column_spec(length, 2 * pairs),
            pl.BlockSpec((None, 2, length, length), lambda d, h, c: (d, h, 0, 0)),
            column_spec(length, 0),
            column_spec(length, 0),
        ],
        pl.BlockSpec((3, None, length, 128), lambda d, h, c: (0, d, 0, h)),
        shape((3, docs, length, columns // 3)),
    )(core, packed, packed, packed, share, delta, mixed)


def gelu_parts(value):
    ratio = 1.0 / (1.0 + tail_spread * jnp.abs(value))
    poly = tail_poly[-1]
    for coefficient in tail_poly[-2::-1]:
        poly = poly * ratio + coefficient
    bell = jnp.exp(-0.5 * value * value)
    tail = poly * ratio * bell
    below = jnp.where(value < 0, tail, 1.0 - tail)
    return value * below, below + value * (bell * 0.3989422804014327)


def up_kernel(core_ref, x_ref, own_ref, other_ref, out_ref, slope_ref):
    def block(weight):
        value, slope = gelu_parts(dot(x_ref[...], weight))
        out_ref[...] = value.astype(low)
        slope_ref[...] = slope.astype(low)

    @pl.when(pl.program_id(0) == 0)
    def _():
        block(own_ref[...])

    @pl.when(pl.program_id(0) == 1)
    def _():
        block(other_ref[...])


def up(x, own, other, core, columns=512, rows=512):
    count, features = x.shape
    half = own.shape[1]
    steps = half // columns
    out = pl.BlockSpec(
        (rows, columns), lambda s, j, i, c: (i, j + steps * jnp.where(s == 0, c[0], 1 - c[0]))
    )
    return call(
        up_kernel,
        "up",
        (2, steps, count // rows),
        [
            pl.BlockSpec((rows, features), lambda s, j, i, c: (i, 0)),
            pl.BlockSpec((features, columns), lambda s, j, i, c: (0, jnp.where(s == 0, j, steps - 1))),
            pl.BlockSpec((features, columns), lambda s, j, i, c: (0, jnp.where(s == 1, j, 0))),
        ],
        [out, out],
        [shape((count, 2 * half))] * 2,
    )(core, x, own, other)


def normalize(value):
    center = value - jnp.mean(value, axis=-1, keepdims=True)
    scale = lax.rsqrt(jnp.mean(center * center, axis=-1, keepdims=True) + eps_norm)
    return center * scale, scale


def normalize_back(scale, unit, delta):
    return scale * (
        delta
        - jnp.mean(delta, axis=-1, keepdims=True)
        - unit * jnp.mean(delta * unit, axis=-1, keepdims=True)
    )


def fetch(own, other, target, sems, core, start=0):
    half = target.shape[1] // 2
    own, other = own.at[:, pl.ds(start, half)], other.at[:, pl.ds(start, half)]
    mine = pl.multiple_of(core * half, 128)
    theirs = pl.multiple_of((1 - core) * half, 128)
    return (
        pltpu.make_async_copy(own, target.at[:, pl.ds(mine, half)], sems.at[0]),
        pltpu.make_async_copy(other, target.at[:, pl.ds(theirs, half)], sems.at[1]),
    )


def merge_kernel(
    core_ref, x_ref, joined_ref, vectors_ref, own_ref, other_ref, sum_ref, low_ref, weight, sems
):
    @pl.when(pl.program_id(0) == 0)
    def _():
        half = weight.shape[1] // 2
        copies = fetch(own_ref, other_ref, weight, sems, core_ref[0], 3 * half)
        for copy in copies:
            copy.start()
        for copy in copies:
            copy.wait()

    total = joined_ref[...] + dot(x_ref[...], weight[...])
    sum_ref[...] = total
    unit, _ = normalize(total)
    low_ref[...] = (unit * vectors_ref[0:1, :] + vectors_ref[1:2, :]).astype(low)


def merge(x, joined, vectors, own, other, core, rows=256):
    count, features = x.shape
    block = pl.BlockSpec((rows, features), lambda i, c: (i, 0))
    return call(
        merge_kernel,
        "merge",
        (count // rows,),
        [
            block,
            block,
            pl.BlockSpec(vectors.shape, lambda i, c: (0, 0)),
            pl.BlockSpec(memory_space=pl.ANY),
            pl.BlockSpec(memory_space=pl.ANY),
        ],
        [block, block],
        [shape((count, features), wide), shape((count, features))],
        [pltpu.VMEM((features, features), low), pltpu.SemaphoreType.DMA((2,))],
    )(core, x, joined, vectors, own, other)


def down_kernel(
    core_ref,
    x_ref,
    sum_ref,
    cotangent_ref,
    vectors_ref,
    own_ref,
    other_ref,
    out_ref,
    delta_ref,
    low_ref,
    sums_ref,
    weight,
    sems,
):
    @pl.when(pl.program_id(0) == 0)
    def _():
        copies = fetch(own_ref, other_ref, weight, sems, core_ref[0])
        for copy in copies:
            copy.start()
        sums_ref[...] = jnp.zeros_like(sums_ref)
        for copy in copies:
            copy.wait()

    unit, _ = normalize(sum_ref[...])
    hidden = unit * vectors_ref[0:1, :] + vectors_ref[1:2, :]
    unit, scale = normalize(hidden + dot(x_ref[...], weight[...]))
    out_ref[...] = unit * vectors_ref[2:3, :] + vectors_ref[3:4, :]
    given = cotangent_ref[...].astype(wide)
    delta = normalize_back(scale, unit, given * vectors_ref[2:3, :])
    delta_ref[...] = delta
    low_ref[...] = delta.astype(low)
    sums_ref[0:1, :] += jnp.sum(given * unit, axis=0, keepdims=True)
    sums_ref[1:2, :] += jnp.sum(given, axis=0, keepdims=True)


def down(x, total, cotangent, vectors, own, other, core, rows=256):
    count, hidden = x.shape
    features = total.shape[1]
    block = pl.BlockSpec((rows, features), lambda i, c: (i, 0))
    return call(
        down_kernel,
        "down",
        (count // rows,),
        [
            pl.BlockSpec((rows, hidden), lambda i, c: (i, 0)),
            block,
            block,
            pl.BlockSpec(vectors.shape, lambda i, c: (0, 0)),
            pl.BlockSpec(memory_space=pl.ANY),
            pl.BlockSpec(memory_space=pl.ANY),
        ],
        [block, block, block, pl.BlockSpec((8, features), lambda i, c: (0, 0))],
        [
            shape((count, features), wide),
            shape((count, features), wide),
            shape((count, features)),
            shape((8, features), wide),
        ],
        [pltpu.VMEM((hidden, features), low), pltpu.SemaphoreType.DMA((2,))],
    )(core, x, total, cotangent, vectors, own, other)


def inner_kernel(
    core_ref,
    low_ref,
    delta_ref,
    slope_ref,
    sum_ref,
    vectors_ref,
    merge_own_ref,
    merge_other_ref,
    down_own_ref,
    down_other_ref,
    up_own_ref,
    up_other_ref,
    inner_ref,
    one_ref,
    one_low_ref,
    mixed_ref,
    sums_ref,
    down_weight,
    up_weight,
    merge_weight,
    sems,
):
    core = core_ref[0]

    def copies():
        return (
            *fetch(down_own_ref, down_other_ref, down_weight, sems.at[0], core),
            *fetch(up_own_ref, up_other_ref, up_weight, sems.at[1], core),
            *fetch(
                merge_own_ref,
                merge_other_ref,
                merge_weight,
                sems.at[2],
                core,
                3 * merge_weight.shape[1] // 2,
            ),
        )

    @pl.when(pl.program_id(0) == 0)
    def _():
        started = copies()
        for copy in started:
            copy.start()
        sums_ref[...] = jnp.zeros_like(sums_ref)
        for copy in started:
            copy.wait()

    inner = (dot(low_ref[...], down_weight[...], NT) * slope_ref[...].astype(wide)).astype(low)
    inner_ref[...] = inner
    delta = delta_ref[...] + dot(inner, up_weight[...], NT)
    unit, scale = normalize(sum_ref[...])
    one = normalize_back(scale, unit, delta * vectors_ref[0:1, :])
    one_ref[...] = one
    one_low = one.astype(low)
    one_low_ref[...] = one_low
    mixed_ref[...] = dot(one_low, merge_weight[...], NT).astype(low)
    sums_ref[0:1, :] += jnp.sum(delta * unit, axis=0, keepdims=True)
    sums_ref[1:2, :] += jnp.sum(delta, axis=0, keepdims=True)


def inner_back(branch, delta, slope, total, vectors, merges, downs, ups, core, rows=256):
    count, hidden = slope.shape
    features = total.shape[1]
    block = pl.BlockSpec((rows, features), lambda i, c: (i, 0))
    tall = pl.BlockSpec((rows, hidden), lambda i, c: (i, 0))
    anywhere = pl.BlockSpec(memory_space=pl.ANY)
    return call(
        inner_kernel,
        "inner_back",
        (count // rows,),
        [
            block,
            block,
            tall,
            block,
            pl.BlockSpec(vectors.shape, lambda i, c: (0, 0)),
            *[anywhere] * 6,
        ],
        [tall, block, block, block, pl.BlockSpec((8, features), lambda i, c: (0, 0))],
        [
            shape((count, hidden)),
            shape((count, features), wide),
            shape((count, features)),
            shape((count, features)),
            shape((8, features), wide),
        ],
        [
            pltpu.VMEM((hidden, features), low),
            pltpu.VMEM((features, hidden), low),
            pltpu.VMEM((features, features), low),
            pltpu.SemaphoreType.DMA((3, 2)),
        ],
    )(core, branch, delta, slope, total, vectors, *merges, *downs, *ups)


def columns_kernel(core_ref, left_ref, own_ref, other_ref, keep_ref, give_ref):
    half = own_ref.shape[-1]
    both = jnp.concatenate([own_ref[...], other_ref[...]], axis=1)
    total = dot(left_ref[...], both, TN)
    keep_ref[...] = total[:, :half].astype(low)
    give_ref[...] = total[:, half:].astype(low)


def into_kernel(core_ref, left_ref, own_ref, other_ref, kept_ref, given_ref, keep_ref, give_ref):
    columns_kernel(core_ref, left_ref, own_ref, other_ref, keep_ref, give_ref)


def weight_into(left, right, keep, give, core):
    count, height = left.shape
    half = right.shape[1] // 2
    last = keep.shape[1] // half - 1
    out = pl.BlockSpec((height, half), lambda i, c: (0, last))
    return call(
        into_kernel,
        "weight_into",
        (1,),
        [
            pl.BlockSpec((count, height), lambda i, c: (0, 0)),
            pl.BlockSpec((count, half), lambda i, c: (0, c[0])),
            pl.BlockSpec((count, half), lambda i, c: (0, 1 - c[0])),
            pl.BlockSpec(memory_space=pl.ANY),
            pl.BlockSpec(memory_space=pl.ANY),
        ],
        [out, out],
        [shape(keep.shape)] * 2,
        aliases={4: 0, 5: 1},
    )(core, left, right, right, keep, give)


def weight_columns(left, right, core, rows=768):
    count, height = left.shape
    parts, _, width = right.shape
    half = width // 2
    steps = height // rows
    out = pl.BlockSpec((rows, half), lambda p, j, c: (j, p))
    return call(
        columns_kernel,
        "weight_columns",
        (parts, steps),
        [
            pl.BlockSpec((count, rows), lambda p, j, c: (0, j)),
            pl.BlockSpec((None, count, half), lambda p, j, c: (p, 0, c[0])),
            pl.BlockSpec((None, count, half), lambda p, j, c: (p, 0, 1 - c[0])),
        ],
        [out, out],
        [shape((height, parts * half))] * 2,
    )(core, left, right, right)


def wide_kernel(core_ref, left_ref, right_ref, keep_ref, give_ref):
    total = dot(left_ref[...], right_ref[...], TN).astype(low)

    @pl.when(pl.program_id(0) == 0)
    def _():
        give_ref[...] = total

    @pl.when(pl.program_id(0) == 1)
    def _():
        keep_ref[...] = total


def weight_wide(left, right, core, spare, columns=768):
    count, height = left.shape
    steps = right.shape[1] // 2 // columns
    return call(
        wide_kernel,
        "weight_wide",
        (2, steps),
        [
            pl.BlockSpec((count, height), lambda s, j, c: (0, 0)),
            pl.BlockSpec(
                (count, columns), lambda s, j, c: (0, j + steps * jnp.where(s == 0, 1 - c[0], c[0]))
            ),
        ],
        [
            pl.BlockSpec((height, columns), lambda s, j, c: (0, jnp.where(s == 1, j, 0))),
            pl.BlockSpec((height, columns), lambda s, j, c: (0, jnp.where(s == 0, j, steps - 1))),
        ],
        [shape((height, right.shape[1] // 2 + spare))] * 2,
    )(core, left, right)


def joined_kernel(core_ref, one_ref, left_ref, right_ref, own_ref, other_ref, out_ref, total):
    part = pl.program_id(1)

    @pl.when(part == 0)
    def _():
        total[...] = one_ref[...]

    both = jnp.concatenate([left_ref[...], right_ref[...]], axis=1)
    weight = jnp.concatenate([own_ref[...], other_ref[...]], axis=1)
    total[...] += dot(both, weight, NT)

    @pl.when(part == pl.num_programs(1) - 1)
    def _():
        out_ref[...] = total[...]


def joined_back(one, packed, own, other, core, rows=1024):
    count, features = one.shape
    parts = packed.shape[0]
    half = features // 2
    block = pl.BlockSpec((rows, features), lambda i, p, c: (i, 0))
    weight = pl.BlockSpec((features, half), lambda i, p, c: (0, p))
    return call(
        joined_kernel,
        "joined_back",
        (count // rows, parts),
        [
            block,
            pl.BlockSpec((None, rows, half), lambda i, p, c: (p, i, c[0])),
            pl.BlockSpec((None, rows, half), lambda i, p, c: (p, i, 1 - c[0])),
            weight,
            weight,
        ],
        block,
        shape((count, features), wide),
        [pltpu.VMEM((rows, features), wide)],
    )(core, one, packed, packed, own, other)


def pool_stats(left, right):
    total, size = left[0] + right[0], left[2] + right[2]
    center = total / size
    apart = (left[1] + right[1]) + (
        left[2] * jnp.square(left[0] / left[2] - center)
        + right[2] * jnp.square(right[0] / right[2] - center)
    )
    return jnp.stack([total, apart, size])


def shards(
    text_rows,
    visual_matrix,
    batch_gain,
    batch_shift,
    attend_weight,
    merge_weight,
    first_gain,
    first_shift,
    up_matrix,
    down_matrix,
    second_gain,
    second_shift,
    segment_counts,
    segment_ids,
    padding_mask,
    cotangent,
):
    docs, length, features = text_rows.shape
    count = docs * length
    hidden = up_matrix.shape[1]
    half = features // 2
    dp, fsdp = lax.axis_size("dp"), lax.axis_size("fsdp")
    core = lax.axis_index("dp") % 2
    which = core.reshape(1).astype(jnp.int32)
    piece = features // fsdp

    small = jnp.stack(
        [first_gain, first_shift, second_gain, second_shift, batch_gain, batch_shift]
    ).reshape(-1)
    first = jnp.concatenate(
        [
            half_of(visual_matrix, core),
            jnp.pad(small, (0, 16 * half - small.size)).reshape(16, half),
        ]
    )
    mine = jnp.concatenate(
        [
            half_of(attend_weight.reshape(piece, 3, features), core).reshape(piece, 3 * half),
            half_of(merge_weight, core),
        ],
        axis=1,
    )
    attend_own = gather_bulk(mine)
    attends = (attend_own, swap(attend_own, "dp", 1))
    first_own = spread(first, "fsdp", None, fsdp)
    first_other = swap(first_own, "dp", 1)
    direct = fsdp == 8
    up_half = half_of(up_matrix, core)
    if direct:
        chip = lax.axis_index("dp") // 2 % 2
        up_column = gather_line(after(half_of(up_half, chip), first_own))
    else:
        up_own = gather_bulk(up_half)
    down_own = gather_bulk(after(half_of(down_matrix, core), first_own))
    full_visual = join(first_own[:, :piece], first_other[:, :piece], core).reshape(features, features)
    small = first_own[:, piece:].reshape(fsdp, 16 * half)[:, : 6 * piece]
    small = small.reshape(fsdp, 6, piece).transpose(1, 0, 2).reshape(6, features)
    vectors = jnp.pad(small.astype(wide), ((0, 2), (0, 0)))
    full_batch_gain, full_batch_shift = vectors[4], vectors[5]

    slot_index = jnp.arange(SEGMAX)
    matches = segment_ids[:, :, None] == slot_index[None, None, :]
    onehot = matches.astype(low)
    onehot_wide = matches.astype(wide)
    divisor = jnp.maximum(jnp.sum(onehot_wide, axis=1), 1.0)[..., None]
    pooled_segments = (
        jnp.einsum("drs,drc->dsc", onehot, text_rows, preferred_element_type=wide) / divisor
    ).astype(low)
    visual_rows = jnp.einsum(
        "bil,ly->biy", pooled_segments, full_visual, preferred_element_type=wide
    )
    valid_slot = (slot_index[None, :] < segment_counts[:, None]).astype(wide)[..., None]
    local_count = jnp.sum(segment_counts).astype(wide)
    local_sum = jnp.sum(valid_slot * visual_rows, axis=(0, 1))
    local_center = visual_rows - local_sum / local_count
    local_square = jnp.sum(valid_slot * local_center * local_center, axis=(0, 1))
    stats = jnp.stack([local_sum, local_square, jnp.full_like(local_sum, local_count)])
    for axis in ("dp", "fsdp"):
        bit = 1
        while bit < lax.axis_size(axis):
            stats = pool_stats(stats, swap(stats, axis, bit))
            bit *= 2
    if direct:
        up_quarter = gather_side(after(up_column, stats))
    segment_total = stats[2]
    batch_center = stats[0] / segment_total
    center = visual_rows - batch_center
    variance = stats[1] / segment_total
    inverse_spread = lax.rsqrt(variance + eps_batch)
    normed = center * inverse_spread
    embedded = (normed * full_batch_gain + full_batch_shift).astype(low)
    joined = text_rows.astype(wide) + jnp.einsum(
        "drs,dsc->drc", onehot, embedded, preferred_element_type=wide
    )
    joined = joined.reshape(count, features)
    joined_low = joined.astype(low)
    if direct:
        joined_low, up_quarter = lax.optimization_barrier((joined_low, up_quarter))
        up_far = swap(up_quarter, "dp", 2)

    packed = project(joined_low, *attends, which).reshape(docs, length, -1)
    attended, share = attend(packed, padding_mask, which)
    flat_attended = attended.reshape(count, features)
    if direct:
        up_own = join(up_quarter, after(up_far, attended), chip)
    total_one, hidden_low = merge(flat_attended, joined, vectors, *attends, which)
    ups = (up_own, swap(up_own, "dp", 1))
    activated, slope = up(hidden_low, *ups, which)
    downs = (down_own, swap(after(down_own, activated), "dp", 1))
    layer_output, delta_two, branch_low, sums_two = down(
        activated, total_one, cotangent.reshape(count, features), vectors, *downs, which
    )

    down_halves = weight_columns(activated, branch_low[None], which)
    down_chip = add_low(down_halves[0], swap(down_halves[1], "dp", 1))
    down_chip, branch_low = lax.optimization_barrier((down_chip, branch_low))
    down_shard = finish(
        lax.psum_scatter(down_chip, "fsdp", scatter_dimension=0, tiled=True), core
    )
    delta_inner, delta_one, one_low, delta_attended, sums_one = inner_back(
        branch_low, delta_two, slope, total_one, vectors, attends, downs, ups, which
    )
    keep, give = weight_wide(hidden_low, delta_inner, which, half)
    keep, give = weight_into(flat_attended, one_low, keep, give, which)
    chip = add_low(keep, swap(give, "dp", 1))
    chip, delta_attended = lax.optimization_barrier((chip, delta_attended))
    up_merge_shard = finish(
        lax.psum_scatter(chip, "fsdp", scatter_dimension=0, tiled=True), core
    )
    delta_packed = attend_back(
        packed, share, delta_attended.reshape(docs, length, features), attended, which
    ).reshape(3, count, features)
    keep, give = weight_columns(joined_low, delta_packed, which)
    keep, give = scatter_begin(add_low(keep, swap(give, "dp", 1)))
    give, delta_packed = lax.optimization_barrier((give, delta_packed))
    given = swap(give, "fsdp", 1)
    delta_joined = joined_back(delta_one, delta_packed, *attends, which)
    attend_shard = scatter_end(keep, given, core)
    delta_joined = delta_joined.reshape(docs, length, features)
    delta_embedded = jnp.einsum(
        "drs,drc->dsc",
        onehot_wide,
        delta_joined,
        precision=highest_precision,
        preferred_element_type=wide,
    )
    sums = jnp.stack(
        [
            sums_one[0],
            sums_one[1],
            sums_two[0],
            sums_two[1],
            jnp.sum(delta_embedded * normed, axis=(0, 1)),
            jnp.sum(delta_embedded, axis=(0, 1)),
        ]
    )
    sums = sum_all(sums)
    gain_total, shift_total = sums[4], sums[5]
    visual_delta_rows = (
        valid_slot
        * full_batch_gain
        * inverse_spread
        * (delta_embedded - shift_total / segment_total - normed * gain_total / segment_total)
    ).astype(low)
    visual_local = jnp.einsum(
        "bli,blz->iz", pooled_segments, visual_delta_rows, preferred_element_type=wide
    ).astype(low)
    visual_shard = scatter_small(half_of(visual_local, core), half_of(visual_local, 1 - core), core)
    delta_pooled = (
        jnp.einsum("zbl,wl->zbw", visual_delta_rows, full_visual, preferred_element_type=wide)
        / divisor
    )
    text_gradient = delta_joined + jnp.einsum(
        "drs,dsc->drc",
        onehot_wide,
        delta_pooled,
        precision=highest_precision,
        preferred_element_type=wide,
    )

    own = lax.dynamic_slice_in_dim(sums, lax.axis_index("fsdp") * piece, piece, 1)
    attend_gradient = join(
        attend_shard[0].reshape(piece, 3, half), attend_shard[1].reshape(piece, 3, half), core
    ).reshape(piece, 3 * features)
    return (
        layer_output.reshape(docs, length, features),
        text_gradient,
        join(*visual_shard, core).astype(wide),
        own[4],
        own[5],
        attend_gradient.astype(wide),
        join(*(part[:, hidden // 2 :] for part in up_merge_shard), core).astype(wide),
        own[0],
        own[1],
        join(*(part[:, : hidden // 2] for part in up_merge_shard), core).astype(wide),
        join(*down_shard, core).astype(wide),
        own[2],
        own[3],
    )


def solution(mesh):
    in_specs = (
        P(("dp", "fsdp"), None, None),
        P("fsdp", None),
        P("fsdp"),
        P("fsdp"),
        P("fsdp", None),
        P("fsdp", None),
        P("fsdp"),
        P("fsdp"),
        P("fsdp", None),
        P("fsdp", None),
        P("fsdp"),
        P("fsdp"),
        P(("dp", "fsdp")),
        P(("dp", "fsdp"), None),
        P(("dp", "fsdp"), None),
        P(("dp", "fsdp"), None, None),
    )
    out_specs = (
        P(("dp", "fsdp"), None, None),
        P(("dp", "fsdp"), None, None),
        P("fsdp", None),
        P("fsdp"),
        P("fsdp"),
        P("fsdp", None),
        P("fsdp", None),
        P("fsdp"),
        P("fsdp"),
        P("fsdp", None),
        P("fsdp", None),
        P("fsdp"),
        P("fsdp"),
    )
    return jax.shard_map(shards, mesh=mesh, in_specs=in_specs, out_specs=out_specs, check_vma=False)
```
